8 devices in a mesh: dp: 1 (over z), cpo: 2 (over y), cp: 4 (over x, core).
Axes of the slice: x: 2, y: 2, z: 1, core: 2. Of those that a mesh axis runs over, the one named last changes fastest.
Arguments:
- queries: bfloat16 [4096, 3, 128], P(('dp', 'cpo', 'cp'))
- keys: bfloat16 [4096, 128], P(('dp', 'cpo', 'cp'))
- values: bfloat16 [4096, 128], P(('dp', 'cpo', 'cp'))
- attn_out: bfloat16 [4096, 3, 128], P(('dp', 'cpo', 'cp'))
- logsumexp: float32 [4096, 3], P(('dp', 'cpo', 'cp'))
- d_out: bfloat16 [4096, 3, 128], P(('dp', 'cpo', 'cp'))
- cu_seqlens: int32 [14], P('dp')
Outputs:
- output 1: bfloat16 [4096, 3, 128], P(('dp', 'cpo', 'cp'))
- output 2: bfloat16 [4096, 128], P(('dp', 'cpo', 'cp'))
- output 3: bfloat16 [4096, 128], P(('dp', 'cpo', 'cp'))
All inputs are finite; a program needn't handle non-finite values.
Results may differ from the reference program's by a relative error of at most 0.001.
Values are sent between devices in bfloat16 or wider.
A program may use at most 1 GiB of HBM per device.

```python
import jax
import jax.numpy as jnp
from jax import lax

CHUNK = 512
GROUP = 8
QHEADS = 3
HEAD_DIM = 128
HOPS = 3
QROWS = 64
SEQ = GROUP * CHUNK
NCUT_RAND = GROUP
NCUT_GRID = GROUP // 3 + 2


def doc_ids(bounds, positions):
    found = jnp.searchsorted(bounds[1:], positions, side="right").astype(jnp.int32)
    return jnp.where((positions >= 0) & (positions < SEQ), found, -1)


def draw_bounds(key):
    key_phase, key_slot, key_cuts = jax.random.split(key, 3)
    span_len = HOPS * CHUNK
    phase = jax.random.randint(key_phase, (), 0, span_len, dtype=jnp.int32)
    grid_cuts = jnp.minimum(phase + span_len * jnp.arange(NCUT_GRID, dtype=jnp.int32), SEQ)
    slot_count = (SEQ - phase) // span_len
    slot = jax.random.randint(key_slot, (), 0, slot_count, dtype=jnp.int32)
    long_start = phase + span_len * slot
    free_cuts = jax.random.randint(key_cuts, (NCUT_RAND,), 1, SEQ, dtype=jnp.int32)
    inside = (free_cuts > long_start) & (free_cuts < long_start + span_len)
    free_cuts = jnp.where(inside, 0, free_cuts)
    every_cut = jnp.concatenate([jnp.zeros((1,), jnp.int32), grid_cuts, free_cuts, jnp.full((1,), SEQ, jnp.int32)])
    return jnp.sort(every_cut).astype(jnp.int32)


def attend_forward(queries, keys, values, ids):
    scale = HEAD_DIM ** -0.5
    span_len = HOPS * CHUNK
    width = span_len + QROWS
    key_pad = jnp.concatenate([jnp.zeros((span_len, HEAD_DIM), jnp.float32), keys.astype(jnp.float32)])
    val_pad = jnp.concatenate([jnp.zeros((span_len, HEAD_DIM), jnp.float32), values.astype(jnp.float32)])
    id_pad = jnp.concatenate([jnp.full((span_len,), -1, jnp.int32), ids])

    def block_fwd(start):
        q_blk = lax.dynamic_slice_in_dim(queries, start, QROWS).astype(jnp.float32)
        id_q = lax.dynamic_slice_in_dim(ids, start, QROWS)
        pos_q = start + jnp.arange(QROWS, dtype=jnp.int32)
        k_blk = lax.dynamic_slice_in_dim(key_pad, start, width)
        v_blk = lax.dynamic_slice_in_dim(val_pad, start, width)
        id_k = lax.dynamic_slice_in_dim(id_pad, start, width)
        pos_k = start - span_len + jnp.arange(width, dtype=jnp.int32)
        keep = (id_q[:, None] == id_k[None, :]) & (pos_k[None, :] <= pos_q[:, None])
        scores = scale * jnp.einsum("qgd,kd->qgk", q_blk, k_blk)
        scores = jnp.where(keep[:, None, :], scores, -1e30)
        top_val = jnp.max(scores, axis=-1, keepdims=True)
        exp_scores = jnp.where(keep[:, None, :], jnp.exp(scores - top_val), 0.0)
        denom = jnp.sum(exp_scores, axis=-1, keepdims=True)
        out_blk = jnp.einsum("qgk,kd->qgd", exp_scores, v_blk) / denom
        return out_blk.astype(jnp.bfloat16), (top_val + jnp.log(denom))[:, :, 0]

    starts = jnp.arange(SEQ // QROWS, dtype=jnp.int32) * QROWS
    out_all, lse_all = lax.map(block_fwd, starts)
    return out_all.reshape(SEQ, QHEADS, HEAD_DIM), lse_all.reshape(SEQ, QHEADS)


def setup_inputs(seed: int = 0, part: int = 0) -> dict:
    part_key = jax.random.fold_in(jax.random.key(seed), part)
    key_q, key_k, key_v, key_do, key_b = jax.random.split(part_key, 5)
    queries = jax.random.normal(key_q, (SEQ, QHEADS, HEAD_DIM), jnp.float32).astype(jnp.bfloat16)
    keys = jax.random.normal(key_k, (SEQ, HEAD_DIM), jnp.float32).astype(jnp.bfloat16)
    values = jax.random.normal(key_v, (SEQ, HEAD_DIM), jnp.float32).astype(jnp.bfloat16)
    d_out = jax.random.normal(key_do, (SEQ, QHEADS, HEAD_DIM), jnp.float32).astype(jnp.bfloat16)
    cu_seqlens = draw_bounds(key_b)
    ids = doc_ids(cu_seqlens, jnp.arange(SEQ, dtype=jnp.int32))
    attn_out, logsumexp = attend_forward(queries, keys, values, ids)
    return {"queries": queries, "keys": keys, "values": values, "attn_out": attn_out, "logsumexp": logsumexp, "d_out": d_out, "cu_seqlens": cu_seqlens}


def reference(queries, keys, values, attn_out, logsumexp, d_out, cu_seqlens):
    scale = HEAD_DIM ** -0.5
    span_len = HOPS * CHUNK
    width = span_len + QROWS
    ids = doc_ids(cu_seqlens, jnp.arange(SEQ, dtype=jnp.int32))
    id_pad = jnp.concatenate([jnp.full((span_len,), -1, jnp.int32), ids])
    key_pad = jnp.concatenate([jnp.zeros((span_len, HEAD_DIM), keys.dtype), keys])
    val_pad = jnp.concatenate([jnp.zeros((span_len, HEAD_DIM), values.dtype), values])
    row_dot = jnp.sum(d_out.astype(jnp.float32) * attn_out.astype(jnp.float32), axis=-1)

    def block_bwd(carry, start):
        dk_acc, dv_acc = carry
        q_blk = lax.dynamic_slice_in_dim(queries, start, QROWS).astype(jnp.float32)
        do_blk = lax.dynamic_slice_in_dim(d_out, start, QROWS).astype(jnp.float32)
        lse_blk = lax.dynamic_slice_in_dim(logsumexp, start, QROWS)
        dot_blk = lax.dynamic_slice_in_dim(row_dot, start, QROWS)
        id_q = lax.dynamic_slice_in_dim(ids, start, QROWS)
        pos_q = start + jnp.arange(QROWS, dtype=jnp.int32)
        k_blk = lax.dynamic_slice_in_dim(key_pad, start, width).astype(jnp.float32)
        v_blk = lax.dynamic_slice_in_dim(val_pad, start, width).astype(jnp.float32)
        id_k = lax.dynamic_slice_in_dim(id_pad, start, width)
        pos_k = start - span_len + jnp.arange(width, dtype=jnp.int32)
        keep = (id_q[:, None] == id_k[None, :]) & (pos_k[None, :] <= pos_q[:, None])
        scores = scale * jnp.einsum("qgd,kd->qgk", q_blk, k_blk)
        p_mat = jnp.where(keep[:, None, :], jnp.exp(scores - lse_blk[:, :, None]), 0.0)
        p_low = p_mat.astype(jnp.bfloat16).astype(jnp.float32)
        dp_mat = jnp.einsum("qgd,kd->qgk", do_blk, v_blk)
        ds_mat = (p_mat * (dp_mat - dot_blk[:, :, None])).astype(jnp.bfloat16).astype(jnp.float32)
        dq_blk = scale * jnp.einsum("qgk,kd->qgd", ds_mat, k_blk)
        dk_part = jnp.einsum("qgk,qgd->kd", ds_mat, q_blk)
        dv_part = jnp.einsum("qgk,qgd->kd", p_low, do_blk)
        dk_acc = lax.dynamic_update_slice_in_dim(dk_acc, lax.dynamic_slice_in_dim(dk_acc, start, width) + dk_part, start, axis=0)
        dv_acc = lax.dynamic_update_slice_in_dim(dv_acc, lax.dynamic_slice_in_dim(dv_acc, start, width) + dv_part, start, axis=0)
        return (dk_acc, dv_acc), dq_blk.astype(jnp.bfloat16)

    init = (jnp.zeros((SEQ + span_len, HEAD_DIM), jnp.float32), jnp.zeros((SEQ + span_len, HEAD_DIM), jnp.float32))
    starts = jnp.arange(SEQ // QROWS, dtype=jnp.int32) * QROWS
    (dk_acc, dv_acc), dq_all = lax.scan(block_bwd, init, starts)
    d_queries = dq_all.reshape(SEQ, QHEADS, HEAD_DIM)
    d_keys = (scale * dk_acc[span_len:]).astype(jnp.bfloat16)
    d_values = dv_acc[span_len:].astype(jnp.bfloat16)
    return d_queries, d_keys, d_values
```

```python
import functools
import math

import jax
import jax.numpy as jnp
from jax import lax
from jax.experimental import pallas as pl
from jax.experimental.pallas import tpu as pltpu
from jax.sharding import PartitionSpec as P

ROWS = 512
HEADS = 3
DIM = 128
CH = 128
NCH = ROWS // CH
NBOUND = 14
LOG2E = math.log2(math.e)
MESH = pl.DeviceIdType.MESH
F32 = jnp.float32
BF16 = jnp.bfloat16
NT = (((1,), (1,)), ((), ()))
TN = (((0,), (0,)), ((), ()))


def device(rank):
    return (0, rank // 4, lax.rem(rank, 4))


def kernel(cu_ref, q_hbm, k_hbm, v_hbm, o_hbm, lse_hbm, do_hbm, dq_ref, dk_ref, dv_ref,
           q_ref, do_ref, o_ref, lse_ref, drow, start_ref, kvown, kvx, kvl, dqt, own,
           mine, theirs, fromsib, xout, lret, xret, rly,
           in_sem, kv_s, kv_r, kx_s, kx_r, re_s, re_r, th_s, th_r, xo_s, xo_r, le_s, le_r, ry_s, ry_r):
    rank = lax.axis_index("cpo") * 4 + lax.axis_index("cp")
    core = lax.rem(rank, 2)
    chip = rank // 2
    sib = rank + 1 - 2 * core
    scale = DIM ** -0.5

    loads = [pltpu.make_async_copy(src, dst, in_sem.at[n]) for n, (src, dst) in enumerate([
        (k_hbm, kvown.at[0]), (v_hbm, kvown.at[1]), (do_hbm, do_ref), (o_hbm, o_ref), (q_hbm, q_ref), (lse_hbm, lse_ref)])]
    for copy in loads:
        copy.start()

    has_l = chip >= 1
    has_r = chip <= 2
    x_from = jnp.where(core == 1, rank - 1, rank - 3)
    x_to = jnp.where(core == 1, rank + 3, rank + 1)
    has_x = x_from >= 0
    x_ret = x_to <= 7

    barrier = pltpu.get_barrier_semaphore()

    def greet(other):
        pl.semaphore_signal(barrier, inc=1, device_id=device(other), device_id_type=MESH)

    greet(sib)
    pl.when(has_l)(lambda: greet(rank - 2))
    pl.when(has_r)(lambda: greet(rank + 2))
    pl.when((core == 1) & (chip <= 1))(lambda: greet(rank + 3))
    pl.when((core == 0) & (chip >= 2))(lambda: greet(rank - 3))
    pl.when(rank == 0)(lambda: greet(4))
    pl.when(rank == 4)(lambda: greet(0))
    one = jnp.int32(1)
    zero = jnp.int32(0)
    count = (one + jnp.where(has_l, one, zero) + jnp.where(has_r, one, zero)
             + jnp.where((core == 1) & (chip <= 1), one, zero) + jnp.where((core == 0) & (chip >= 2), one, zero)
             + jnp.where(rank == 0, one, zero) + jnp.where(rank == 4, one, zero))
    pl.semaphore_wait(barrier, count)

    def remote(src, dst, s_sem, r_sem, other):
        return pltpu.make_async_remote_copy(src_ref=src, dst_ref=dst, send_sem=s_sem, recv_sem=r_sem,
                                            device_id=device(other), device_id_type=MESH)

    def rows(i):
        return pl.ds(pl.multiple_of(i * CH, CH), CH)

    def kv_right(i):
        return remote(kvown.at[:, rows(i)], kvl.at[core, :, rows(i)], kv_s.at[i], kv_r.at[i], rank + 2)

    def kv_x(i):
        return remote(kvown.at[:, rows(i)], kvx.at[:, rows(i)], kx_s.at[i], kx_r.at[i], x_to)

    def kv_relay(i):
        return remote(kvl.at[core, :, rows(i)], kvl.at[core, :, rows(i)], re_s.at[i], re_r.at[i], sib)

    def kv_relayed(i):
        return remote(kvl.at[1 - core, :, rows(i)], kvl.at[1 - core, :, rows(i)], re_s.at[i], re_r.at[i], sib)

    def give_sib(i):
        return remote(theirs.at[i], fromsib.at[i], th_s.at[i], th_r.at[i], sib)

    def give_x(i):
        return remote(xout.at[i], xret.at[i], xo_s.at[i], xo_r.at[i], x_from)

    def give_left(i):
        return remote(mine.at[i], lret.at[i], le_s.at[i], le_r.at[i], rank - 2)

    def give_relay(i):
        return remote(mine.at[i], rly.at[i], le_s.at[i], ry_r.at[i], 0)

    def pass_on(i):
        return remote(rly.at[i], lret.at[i], ry_s.at[i], le_r.at[i], 2)

    loads[0].wait()
    loads[1].wait()

    def send_kv(i, _):
        pl.when(has_r)(lambda: kv_right(i).start())
        pl.when(x_ret)(lambda: kv_x(i).start())
        return 0

    lax.fori_loop(0, NCH, send_kv, 0)

    pos = rank * ROWS + lax.broadcasted_iota(jnp.int32, (1, ROWS), 1)
    start = jnp.zeros((1, ROWS), jnp.int32)
    for n in range(NBOUND):
        bound = cu_ref[n]
        start = jnp.where(bound <= pos, bound, start)
    start_ref[0:1, :] = start

    loads[2].wait()
    loads[3].wait()
    for g in range(HEADS):
        prod = do_ref[g].astype(F32) * o_ref[g].astype(F32)
        drow[g:g + 1, :] = jnp.sum(prod.T, axis=0, keepdims=True)
    loads[4].wait()
    loads[5].wait()

    def part(kv, i, first_key, diag):
        k = kv[0, rows(i), :]
        v = kv[1, rows(i), :]
        key = first_key + i * CH + lax.broadcasted_iota(jnp.int32, (CH, ROWS), 0)
        keep = key >= start_ref[0:1, :]
        if diag:
            keep = keep & (key <= rank * ROWS + lax.broadcasted_iota(jnp.int32, (CH, ROWS), 1))
        dk = dv = None
        for g in range(HEADS):
            q, do = q_ref[g], do_ref[g]
            s = lax.dot_general(k, q, NT, preferred_element_type=F32)
            p = jnp.exp2(s * (scale * LOG2E) - lse_ref[g:g + 1, :] * LOG2E)
            p = jnp.where(keep, p, 0.0)
            dp = lax.dot_general(v, do, NT, preferred_element_type=F32)
            ds = (p * (dp - drow[g:g + 1, :])).astype(BF16)
            dv_g = jnp.dot(p.astype(BF16), do, preferred_element_type=F32)
            dk_g = jnp.dot(ds, q, preferred_element_type=F32)
            dk, dv = (dk_g, dv_g) if dk is None else (dk + dk_g, dv + dv_g)
            dqt[g] += lax.dot_general(k, ds, TN, preferred_element_type=F32)
        return dk, dv

    dqt[...] = jnp.zeros_like(dqt)

    def diag_step(i, _):
        dk, dv = part(kvown, i, rank * ROWS, True)
        own[i, 0] = dk
        own[i, 1] = dv
        return 0

    lax.fori_loop(0, NCH, diag_step, 0)

    def step(i, _):
        @pl.when(has_l)
        def _():
            kv_right(i).wait_recv()
            kv_relay(i).start()
            dk, dv = part(kvl.at[core], i, (rank - 2) * ROWS, False)
            mine[i, 0] = dk
            mine[i, 1] = dv
            kv_relayed(i).wait_recv()
            dk, dv = part(kvl.at[1 - core], i, (sib - 2) * ROWS, False)
            theirs[i, 0] = dk
            theirs[i, 1] = dv
            give_sib(i).start()

        @pl.when(has_x)
        def _():
            kv_x(i).wait_recv()
            dk, dv = part(kvx, i, x_from * ROWS, False)
            xout[i, 0] = dk
            xout[i, 1] = dv
            give_x(i).start()

        @pl.when(has_l)
        def _():
            give_sib(i).wait_recv()
            mine[i] += fromsib[i]
            pl.when(rank != 4)(lambda: give_left(i).start())
            pl.when(rank == 4)(lambda: give_relay(i).start())

        return 0

    lax.fori_loop(0, NCH, step, 0)

    @pl.when(rank == 0)
    def _():
        def fwd(i, _):
            give_relay(i).wait_recv()
            pass_on(i).start()
            return 0
        lax.fori_loop(0, NCH, fwd, 0)

    for g in range(HEADS):
        dq_ref[g] = (dqt[g].T * scale).astype(BF16)

    def finish(i, _):
        @pl.when(x_ret)
        def _():
            give_x(i).wait_recv()
            own[i] += xret[i]

        @pl.when(has_r)
        def _():
            give_left(i).wait_recv()
            own[i] += lret[i]

        dk_ref[rows(i), :] = (own[i, 0] * scale).astype(BF16)
        dv_ref[rows(i), :] = own[i, 1].astype(BF16)
        return 0

    lax.fori_loop(0, NCH, finish, 0)

    def drain(i, _):
        pl.when(has_r)(lambda: kv_right(i).wait_send())
        pl.when(x_ret)(lambda: kv_x(i).wait_send())

        @pl.when(has_l)
        def _():
            kv_relay(i).wait_send()
            give_sib(i).wait_send()
            give_left(i).wait_send()

        pl.when(has_x)(lambda: give_x(i).wait_send())
        pl.when(rank == 0)(lambda: pass_on(i).wait_send())
        return 0

    lax.fori_loop(0, NCH, drain, 0)


def solution(mesh):
    def local(queries, keys, values, attn_out, logsumexp, d_out, cu_seqlens):
        rows, heads, head = queries.shape
        swap = lambda a: jnp.transpose(a, (1, 0, 2))
        big = pltpu.VMEM((heads, rows, head), BF16)
        kv = pltpu.VMEM((2, rows, head), BF16)
        sums = pltpu.VMEM((NCH, 2, CH, head), F32)
        sem = pltpu.SemaphoreType.DMA((NCH,))
        anyspec = pl.BlockSpec(memory_space=pl.ANY)
        vspec = pl.BlockSpec(memory_space=pltpu.VMEM)
        dq, dk, dv = pl.pallas_call(
            kernel,
            out_shape=(jax.ShapeDtypeStruct((heads, rows, head), BF16),
                       jax.ShapeDtypeStruct((rows, head), BF16),
                       jax.ShapeDtypeStruct((rows, head), BF16)),
            in_specs=[pl.BlockSpec(memory_space=pltpu.SMEM)] + [anyspec] * 6,
            out_specs=(vspec, vspec, vspec),
            scratch_shapes=[big, big, big, pltpu.VMEM((heads, rows), F32), pltpu.VMEM((8, rows), F32),
                            pltpu.VMEM((8, rows), jnp.int32), kv, kv, pltpu.VMEM((2, 2, rows, head), BF16),
                            pltpu.VMEM((heads, head, rows), F32), sums,
                            sums, sums, sums, sums, sums, sums, sums,
                            pltpu.SemaphoreType.DMA((6,))] + [sem] * 14,
            compiler_params=pltpu.CompilerParams(collective_id=0, has_side_effects=True,
                                                 vmem_limit_bytes=48 << 20),
        )(cu_seqlens, swap(queries), keys, values, swap(attn_out), logsumexp.T, swap(d_out))
        return jnp.transpose(dq, (1, 0, 2)), dk, dv

    seq = P(("dp", "cpo", "cp"))
    return jax.shard_map(local, mesh=mesh, in_specs=(seq,) * 6 + (P("dp"),), out_specs=(seq, seq, seq), check_vma=False)
```

```python
import functools
import math

import jax
import jax.numpy as jnp
from jax import lax
from jax.experimental import pallas as pl
from jax.experimental.pallas import tpu as pltpu
from jax.sharding import PartitionSpec as P

ROWS = 512
HEADS = 3
DIM = 128
CH = 128
NCH = ROWS // CH
NBOUND = 14
QALL = HEADS * ROWS
LOG2E = math.log2(math.e)
MESH = pl.DeviceIdType.MESH
F32 = jnp.float32
BF16 = jnp.bfloat16
NT = (((1,), (1,)), ((), ()))
TN = (((0,), (0,)), ((), ()))


def device(rank):
    return (0, rank >> 2, rank & 3)


def kernel(cu_hbm, q_hbm, k_hbm, v_hbm, o_hbm, lse_hbm, do_hbm, dq_ref, dk_ref, dv_ref,
           cu_ref, q_ref, do_ref, o_ref, lse_ref, lrow, drow, start_ref, kvown, kvx, kvl, dqt, own,
           mine, theirs, fromsib, xout, lret, xret, rly,
           in_sem, kv_s, kv_r, kx_s, kx_r, re_s, re_r, th_s, th_r, xo_s, xo_r, le_s, le_r, ry_s, ry_r):
    rank = lax.axis_index("cpo") * 4 + lax.axis_index("cp")
    core = rank & 1
    chip = rank >> 1
    sib = rank + 1 - 2 * core
    scale = DIM ** -0.5

    has_l = chip >= 1
    has_r = chip <= 2
    x_from = jnp.where(core == 1, rank - 1, rank - 3)
    x_to = jnp.where(core == 1, rank + 3, rank + 1)
    has_x = x_from >= 0
    x_ret = x_to <= 7

    barrier = pltpu.get_barrier_semaphore()

    def greet(other):
        pl.semaphore_signal(barrier, inc=1, device_id=device(other), device_id_type=MESH)

    greet(sib)
    pl.when(has_l)(lambda: greet(rank - 2))
    pl.when(has_r)(lambda: greet(rank + 2))
    pl.when((core == 1) & (chip <= 1))(lambda: greet(rank + 3))
    pl.when((core == 0) & (chip >= 2))(lambda: greet(rank - 3))
    pl.when(rank == 0)(lambda: greet(4))
    pl.when(rank == 4)(lambda: greet(0))
    loads = [pltpu.make_async_copy(src, dst, in_sem.at[n]) for n, (src, dst) in enumerate([
        (k_hbm, kvown.at[0]), (v_hbm, kvown.at[1]), (do_hbm, do_ref), (o_hbm, o_ref), (q_hbm, q_ref), (lse_hbm, lse_ref), (cu_hbm, cu_ref)])]
    for copy in loads:
        copy.start()

    one = jnp.int32(1)
    zero = jnp.int32(0)
    count = (one + jnp.where(has_l, one, zero) + jnp.where(has_r, one, zero)
             + jnp.where((core == 1) & (chip <= 1), one, zero) + jnp.where((core == 0) & (chip >= 2), one, zero)
             + jnp.where(rank == 0, one, zero) + jnp.where(rank == 4, one, zero))
    pl.semaphore_wait(barrier, count)

    def remote(src, dst, s_sem, r_sem, other):
        return pltpu.make_async_remote_copy(src_ref=src, dst_ref=dst, send_sem=s_sem, recv_sem=r_sem,
                                            device_id=device(other), device_id_type=MESH)

    def rows(i):
        return pl.ds(pl.multiple_of(i * CH, CH), CH)

    def kv_right(i):
        return remote(kvown.at[:, rows(i)], kvl.at[core, :, rows(i)], kv_s.at[i], kv_r.at[i], rank + 2)

    def kv_x(i):
        return remote(kvown.at[:, rows(i)], kvx.at[:, rows(i)], kx_s.at[i], kx_r.at[i], x_to)

    def kv_relay(i):
        return remote(kvl.at[core, :, rows(i)], kvl.at[core, :, rows(i)], re_s.at[i], re_r.at[i], sib)

    def kv_relayed(i):
        return remote(kvl.at[1 - core, :, rows(i)], kvl.at[1 - core, :, rows(i)], re_s.at[i], re_r.at[i], sib)

    def give_sib(i):
        return remote(theirs.at[i], fromsib.at[i], th_s.at[i], th_r.at[i], sib)

    def give_x(i):
        return remote(xout.at[i], xret.at[i], xo_s.at[i], xo_r.at[i], x_from)

    def give_left(i):
        return remote(mine.at[i], lret.at[i], le_s.at[i], le_r.at[i], rank - 2)

    def give_relay(i):
        return remote(mine.at[i], rly.at[i], le_s.at[i], ry_r.at[i], 0)

    def pass_on(i):
        return remote(rly.at[i], lret.at[i], ry_s.at[i], le_r.at[i], 2)

    loads[0].wait()
    loads[1].wait()

    def send_kv(i, _):
        pl.when(has_r)(lambda: kv_right(i).start())
        pl.when(x_ret)(lambda: kv_x(i).start())
        return 0

    lax.fori_loop(0, NCH, send_kv, 0)

    pos = rank * ROWS + lax.broadcasted_iota(jnp.int32, (1, ROWS), 1)
    start = jnp.zeros((1, ROWS), jnp.int32)
    loads[6].wait()
    for n in range(NBOUND):
        bound = cu_ref[n]
        start = jnp.where(bound <= pos, bound, start)

    loads[2].wait()
    loads[3].wait()
    loads[5].wait()
    for g in range(HEADS):
        lanes = slice(g * ROWS, (g + 1) * ROWS)
        prod = do_ref[lanes].astype(F32) * o_ref[lanes].astype(F32)
        drow[0:1, lanes] = jnp.sum(prod.T, axis=0, keepdims=True)
        lrow[0:1, lanes] = lse_ref[g:g + 1, :] * LOG2E
        start_ref[0:1, lanes] = start
    loads[4].wait()

    def part(kv, i, first_key, diag):
        k = kv[0, rows(i), :]
        v = kv[1, rows(i), :]
        q, do = q_ref[...], do_ref[...]
        key = first_key + i * CH + lax.broadcasted_iota(jnp.int32, (CH, QALL), 0)
        keep = key >= start_ref[0:1, :]
        if diag:
            keep = keep & (key - rank * ROWS <= lax.rem(lax.broadcasted_iota(jnp.int32, (CH, QALL), 1), ROWS))
        s = lax.dot_general(k, q, NT, preferred_element_type=F32)
        dp = lax.dot_general(v, do, NT, preferred_element_type=F32)
        p = jnp.exp2(s * (scale * LOG2E) - lrow[0:1, :])
        p = jnp.where(keep, p, 0.0)
        ds = (p * (dp - drow[0:1, :])).astype(BF16)
        dv = jnp.dot(p.astype(BF16), do, preferred_element_type=F32)
        dk = jnp.dot(ds, q, preferred_element_type=F32)
        dqt[...] += lax.dot_general(k, ds, TN, preferred_element_type=F32)
        return dk, dv

    dqt[...] = jnp.zeros_like(dqt)

    def diag_step(i, _):
        dk, dv = part(kvown, i, rank * ROWS, True)
        own[i, 0] = dk
        own[i, 1] = dv
        return 0

    lax.fori_loop(0, NCH, diag_step, 0)

    @pl.when(has_l)
    def _():
        kv_right(0).wait_recv()
        kv_relay(0).start()

        def step(i, _):
            kv_relayed(i).wait_recv()
            dk, dv = part(kvl.at[1 - core], i, (sib - 2) * ROWS, False)
            theirs[i, 0] = dk
            theirs[i, 1] = dv
            give_sib(i).start()

            @pl.when(i + 1 < NCH)
            def _():
                kv_right(i + 1).wait_recv()
                kv_relay(i + 1).start()

            dk, dv = part(kvl.at[core], i, (rank - 2) * ROWS, False)
            give_sib(i).wait_recv()
            mine[i, 0] = dk + fromsib[i, 0]
            mine[i, 1] = dv + fromsib[i, 1]
            pl.when(rank != 4)(lambda: give_left(i).start())
            pl.when(rank == 4)(lambda: give_relay(i).start())
            return 0

        lax.fori_loop(0, NCH, step, 0)

    @pl.when(has_x)
    def _():
        def xstep(i, _):
            kv_x(i).wait_recv()
            dk, dv = part(kvx, i, x_from * ROWS, False)
            xout[i, 0] = dk
            xout[i, 1] = dv
            give_x(i).start()
            return 0

        lax.fori_loop(0, NCH, xstep, 0)

    @pl.when(rank == 0)
    def _():
        def fwd(i, _):
            give_relay(i).wait_recv()
            pass_on(i).start()
            return 0
        lax.fori_loop(0, NCH, fwd, 0)

    for g in range(HEADS):
        lanes = slice(g * ROWS, (g + 1) * ROWS)
        dq_ref[lanes] = (dqt[:, lanes].T * scale).astype(BF16)

    def finish(i, _):
        @pl.when(x_ret)
        def _():
            give_x(i).wait_recv()
            own[i] += xret[i]

        @pl.when(has_r)
        def _():
            give_left(i).wait_recv()
            own[i] += lret[i]

        dk_ref[rows(i), :] = (own[i, 0] * scale).astype(BF16)
        dv_ref[rows(i), :] = own[i, 1].astype(BF16)
        return 0

    lax.fori_loop(0, NCH, finish, 0)

    def drain(i, _):
        pl.when(has_r)(lambda: kv_right(i).wait_send())
        pl.when(x_ret)(lambda: kv_x(i).wait_send())

        @pl.when(has_l)
        def _():
            kv_relay(i).wait_send()
            give_sib(i).wait_send()
            give_left(i).wait_send()

        pl.when(has_x)(lambda: give_x(i).wait_send())
        pl.when(rank == 0)(lambda: pass_on(i).wait_send())
        return 0

    lax.fori_loop(0, NCH, drain, 0)


def write_out(dq_ref, dk_ref, dv_ref, dq_hbm, dk_hbm, dv_hbm, sem):
    copies = [pltpu.make_async_copy(src, dst, sem.at[n]) for n, (src, dst) in enumerate([
        (dq_ref, dq_hbm), (dk_ref, dk_hbm), (dv_ref, dv_hbm)])]
    for copy in copies:
        copy.start()
    for copy in copies:
        copy.wait()


def solution(mesh):
    def local(queries, keys, values, attn_out, logsumexp, d_out, cu_seqlens):
        rows, heads, head = queries.shape
        swap = lambda a: jnp.transpose(a, (1, 0, 2)).reshape(heads * rows, head)
        big = pltpu.VMEM((QALL, head), BF16)
        kv = pltpu.VMEM((2, rows, head), BF16)
        sums = pltpu.VMEM((NCH, 2, CH, head), F32)
        sem = pltpu.SemaphoreType.DMA((NCH,))
        anyspec = pl.BlockSpec(memory_space=pl.ANY)
        vspec = pl.BlockSpec(memory_space=pltpu.VMEM)
        dq, dk, dv = pl.pallas_call(
            kernel,
            out_shape=(pltpu.VMEM((QALL, head), BF16), pltpu.VMEM((rows, head), BF16), pltpu.VMEM((rows, head), BF16)),
            in_specs=[anyspec] * 7,
            out_specs=(vspec, vspec, vspec),
            scratch_shapes=[pltpu.SMEM((NBOUND,), jnp.int32), big, big, big, pltpu.VMEM((heads, rows), F32), pltpu.VMEM((8, QALL), F32),
                            pltpu.VMEM((8, QALL), F32), pltpu.VMEM((8, QALL), jnp.int32), kv, kv, pltpu.VMEM((2, 2, rows, head), BF16),
                            pltpu.VMEM((head, QALL), F32), sums,
                            sums, sums, sums, sums, sums, sums, sums,
                            pltpu.SemaphoreType.DMA((7,))] + [sem] * 14,
            compiler_params=pltpu.CompilerParams(collective_id=0, has_side_effects=True,
                                                 vmem_limit_bytes=48 << 20),
        )(*[pltpu.with_memory_space_constraint(a, pltpu.HBM) for a in (
            cu_seqlens, swap(queries), keys, values, swap(attn_out), logsumexp.T, swap(d_out))])
        dq, dk, dv = pl.pallas_call(
            write_out,
            out_shape=(jax.ShapeDtypeStruct(dq.shape, BF16), jax.ShapeDtypeStruct(dk.shape, BF16),
                       jax.ShapeDtypeStruct(dv.shape, BF16)),
            in_specs=[vspec] * 3,
            out_specs=(anyspec,) * 3,
            scratch_shapes=[pltpu.SemaphoreType.DMA((3,))],
            compiler_params=pltpu.CompilerParams(vmem_limit_bytes=4 << 20),
        )(dq, dk, dv)
        return jnp.transpose(dq.reshape(heads, rows, head), (1, 0, 2)), dk, dv

    seq = P(("dp", "cpo", "cp"))
    return jax.shard_map(local, mesh=mesh, in_specs=(seq,) * 6 + (P("dp"),), out_specs=(seq, seq, seq), check_vma=False)
```

```python
import math

import jax
import jax.numpy as jnp
from jax import lax
from jax.experimental import pallas as pl
from jax.experimental.pallas import tpu as pltpu
from jax.sharding import PartitionSpec as P

ROWS = 512
HEADS = 3
DIM = 128
NBOUND = 14
QALL = HEADS * ROWS
XCH = 256
NX = ROWS // XCH
LSIZE = (64, 64, 128, 128, 128)
LOFF = (0, 64, 128, 256, 384)
NL = len(LSIZE)
NRLY = 4
STEPS = tuple(zip(LOFF, LSIZE))
LOG2E = math.log2(math.e)
MESH = pl.DeviceIdType.MESH
F32 = jnp.float32
BF16 = jnp.bfloat16
NT = (((1,), (1,)), ((), ()))
TN = (((0,), (0,)), ((), ()))


def device(rank):
    return (0, rank >> 2, rank & 3)


def kernel(cu_hbm, q_hbm, k_hbm, v_hbm, o_hbm, lse_hbm, do_hbm, dq_ref, dk_ref, dv_ref,
           cu_ref, qd, row, qfar, rfar, o_ref, lse_ref, kvown, kvx, kvl, kvb, dqt, own, mine, xout, lret, xret, rly,
           in_sem, sb_s, sb_r, kv_s, kv_r, re_s, re_r, le_s, le_r, ry_s, ry_r, kx_s, kx_r, xo_s, xo_r, bn_s, bn_r):
    rank = lax.axis_index("cpo") * 4 + lax.axis_index("cp")
    core = rank & 1
    chip = rank >> 1
    sib = rank + 1 - 2 * core
    scale = DIM ** -0.5

    loads = [pltpu.make_async_copy(src, dst, in_sem.at[n]) for n, (src, dst) in enumerate([
        (k_hbm, kvown.at[0]), (v_hbm, kvown.at[1]), (do_hbm, qd.at[0, 1]), (q_hbm, qd.at[0, 0]), (o_hbm, o_ref),
        (lse_hbm, lse_ref), (cu_hbm, cu_ref)])]
    loads[0].start()
    loads[1].start()

    has_l = chip >= 1
    has_r = chip <= 2
    x_from = jnp.where(core == 1, rank - 1, rank - 3)
    x_to = jnp.where(core == 1, rank + 3, rank + 1)
    has_x = x_from >= 0
    x_ret = x_to <= 7

    barrier = pltpu.get_barrier_semaphore()

    def greet(other):
        pl.semaphore_signal(barrier, inc=1, device_id=device(other), device_id_type=MESH)

    far_right = (core == 1) & (chip <= 1)
    far_left = (core == 0) & (chip >= 2)
    pl.when(has_l)(lambda: greet(rank - 2))
    pl.when(has_r)(lambda: greet(rank + 2))
    pl.when(far_right)(lambda: greet(rank + 3))
    pl.when(far_left)(lambda: greet(rank - 3))
    pl.when(chip == 1)(lambda: greet(rank + 4))
    pl.when(chip == 3)(lambda: greet(rank - 4))
    pl.when(rank == 0)(lambda: greet(4))
    pl.when(rank == 4)(lambda: greet(0))
    greet(sib)
    for copy in loads[2:]:
        copy.start()
    one = jnp.int32(1)
    zero = jnp.int32(0)
    count = one
    for there in (has_l, has_r, far_right, far_left, chip == 1, chip == 3, rank == 0, rank == 4):
        count = count + jnp.where(there, one, zero)
    pl.semaphore_wait(barrier, count)

    def remote(src, dst, s_sem, r_sem, other):
        return pltpu.make_async_remote_copy(src_ref=src, dst_ref=dst, send_sem=s_sem, recv_sem=r_sem,
                                            device_id=device(other), device_id_type=MESH)

    def rows(off, size):
        return pl.ds(off, size)

    def lend(src, dst, n, other):
        return remote(src, dst, sb_s.at[n], sb_r.at[n], other)

    def kv_right(i, off, size):
        return remote(kvown.at[:, rows(off, size)], kvl.at[core, :, rows(off, size)], kv_s.at[i], kv_r.at[i], rank + 2)

    last = pl.ds(LOFF[-1], LSIZE[-1])

    def bounce():
        return remote(kvown.at[:, last], kvb, kv_s.at[NL - 1], bn_r.at[0], rank + 4)

    def bounce_on():
        return remote(kvb, kvl.at[core, :, last], bn_s.at[0], kv_r.at[NL - 1], rank - 2)

    def kv_relay(i, off, size):
        return remote(kvl.at[core, :, rows(off, size)], kvl.at[core, :, rows(off, size)], re_s.at[i], re_r.at[i], sib)

    def kv_relayed(i, off, size):
        part = kvl.at[1 - core, :, rows(off, size)]
        return remote(part, part, re_s.at[i], re_r.at[i], sib)

    def kv_x(i):
        return remote(kvown.at[:, rows(i * XCH, XCH)], kvx.at[:, rows(i * XCH, XCH)], kx_s.at[i], kx_r.at[i], x_to)

    def give_x():
        return remote(xout, xret, xo_s.at[0], xo_r.at[0], rank - 3)

    def give_left(i, off, size):
        return remote(mine.at[:, rows(off, size)], lret.at[:, rows(off, size)], le_s.at[i], le_r.at[i], rank - 2)

    def give_relay(i, off, size):
        return remote(mine.at[:, rows(off, size)], rly.at[:, rows(off, size)], le_s.at[i], ry_r.at[i], 0)

    def pass_on(i, off, size):
        return remote(rly.at[:, rows(off, size)], lret.at[:, rows(off, size)], ry_s.at[i], le_r.at[i], 2)

    loads[0].wait()
    loads[1].wait()

    @pl.when(has_r)
    def _():
        pl.when(chip == 1)(lambda: bounce().start())
        for i in range(NL - 1):
            kv_right(i, LOFF[i], LSIZE[i]).start()
        pl.when(chip != 1)(lambda: kv_right(NL - 1, LOFF[-1], LSIZE[-1]).start())

    loads[2].wait()
    loads[3].wait()
    sib_qd, sib_row = lend(qd.at[0], qd.at[1], 0, sib), lend(row.at[0], row.at[1], 1, sib)
    far_to = jnp.where(core == 0, rank - 3, rank + 3)
    far_qd, far_row = lend(qd.at[0, :, :, 0:XCH], qfar, 2, far_to), lend(rfar.at[0], rfar.at[1], 3, far_to)
    sib_qd.start()
    pl.when(far_left)(lambda: far_qd.start())

    pos = rank * ROWS + lax.broadcasted_iota(jnp.int32, (1, ROWS), 1)
    start = jnp.zeros((1, ROWS), jnp.int32)
    loads[6].wait()
    for n in range(NBOUND):
        bound = cu_ref[n]
        start = jnp.where(bound <= pos, bound, start)
    loads[4].wait()
    loads[5].wait()
    for g in range(HEADS):
        lanes = slice(g * ROWS, (g + 1) * ROWS)
        prod = qd[0, 1, g].astype(F32) * o_ref[g].astype(F32)
        half = slice(g * XCH, (g + 1) * XCH)
        for n, line in enumerate([lse_ref[g:g + 1, :] * LOG2E, jnp.sum(prod.T, axis=0, keepdims=True), start.astype(F32)]):
            row[0, n:n + 1, lanes] = line
            rfar[0, n:n + 1, half] = line[:, 0:XCH]
    sib_row.start()
    pl.when(far_left)(lambda: far_row.start())

    def lines(ref, spans):
        return [jnp.concatenate([ref[n:n + 1, span] for span in spans], axis=1) for n in range(3)]

    def queries(who):
        return [qd[who, n].reshape(QALL, DIM) for n in range(2)] + [row[who, n:n + 1, :] for n in range(3)]

    def own_rows(lo, hi):
        q, do = (qd[0, n, :, lo:hi].reshape(HEADS * (hi - lo), DIM) for n in range(2))
        return [q, do] + lines(row.at[0], [slice(g * ROWS + lo, g * ROWS + hi) for g in range(HEADS)])

    def part(query, kv, off, size, first_key, low=None, dq_rows=None, want_kv=True):
        q, do, lse, dot, start = query
        k = kv[0, off:off + size, :]
        v = kv[1, off:off + size, :]
        width = q.shape[0]
        key = lax.broadcasted_iota(jnp.int32, (size, width), 0)
        keep = (first_key + off + key).astype(F32) >= start
        if low is not None:
            keep = keep & (key <= lax.rem(lax.broadcasted_iota(jnp.int32, (size, width), 1), ROWS - low))
        s = lax.dot_general(k, q, NT, preferred_element_type=F32)
        dp = lax.dot_general(v, do, NT, preferred_element_type=F32)
        p = jnp.exp2(s * (scale * LOG2E) - lse)
        p = jnp.where(keep, p, 0.0)
        ds = (p * (dp - dot)).astype(BF16)
        if dq_rows is not None:
            lo, hi = dq_rows
            dq = lax.dot_general(k, ds, TN, preferred_element_type=F32)
            if low == 0:
                dqt[...] = dq
            elif hi - lo == ROWS:
                dqt[...] += dq
            else:
                for g in range(HEADS):
                    dqt[:, g * ROWS + lo:g * ROWS + hi] += dq[:, g * (hi - lo):(g + 1) * (hi - lo)]
        if want_kv:
            dv = jnp.dot(p.astype(BF16), do, preferred_element_type=F32)
            dk = jnp.dot(ds, q, preferred_element_type=F32)
            return dk, dv

    everything = (0, ROWS)

    for off in range(0, ROWS, XCH):
        dk, dv = part(own_rows(off, ROWS), kvown, off, XCH, rank * ROWS, low=off, dq_rows=(off, ROWS))
        own[0, off:off + XCH] = dk
        own[1, off:off + XCH] = dv

    pl.when(x_ret)(lambda: [kv_x(i).start() for i in range(NX)] and None)

    def lstep(n):
        off, size = STEPS[n]
        pieces = [(i, LOFF[i], LSIZE[i]) for i in range(NL) if off <= LOFF[i] < off + size]
        for piece in pieces:
            kv_right(*piece).wait_recv()
            kv_relay(*piece).start()
        mine_kv = kvl.at[core]
        dk, dv = part(queries(0), mine_kv, off, size, (rank - 2) * ROWS, dq_rows=everything)
        if n == 0:
            @pl.when(rank != 4)
            def _():
                sib_qd.wait_recv()
                sib_row.wait_recv()
        dk2, dv2 = part(queries(1), mine_kv, off, size, (rank - 2) * ROWS)
        mine[0, off:off + size] = dk + dk2
        mine[1, off:off + size] = dv + dv2

        @pl.when(rank != 4)
        def _():
            for piece in pieces:
                give_left(*piece).start()

        @pl.when(rank == 4)
        def _():
            for piece in pieces:
                (give_relay if piece[0] < NRLY else give_left)(*piece).start()

    def sib_keys(off):
        dk, dv = part(queries(1), kvown, off, XCH, rank * ROWS)
        own[0, off:off + XCH] += dk
        own[1, off:off + XCH] += dv

    @pl.when(rank == 4)
    def _():
        sib_qd.wait_recv()
        sib_row.wait_recv()
        sib_keys(0)

    @pl.when(chip == 3)
    def _():
        bounce().wait_recv()
        bounce_on().start()

    @pl.when(has_l)
    def _():
        for n in range(len(STEPS)):
            lstep(n)

    @pl.when(far_left)
    def _():
        kv_x(1).wait_recv()
        dk, dv = part(queries(0), kvx, XCH, XCH, x_from * ROWS, dq_rows=everything)
        xout[0] = dk
        xout[1] = dv
        give_x().start()
        kv_x(0).wait_recv()
        part(own_rows(0, XCH), kvx, 0, XCH, x_from * ROWS, dq_rows=(0, XCH), want_kv=False)

    @pl.when(has_l)
    def _():
        for off in range(0, ROWS, XCH):
            for i in range(NL):
                if off <= LOFF[i] < off + XCH:
                    kv_relayed(i, LOFF[i], LSIZE[i]).wait_recv()
            part(queries(0), kvl.at[1 - core], off, XCH, (sib - 2) * ROWS, dq_rows=everything, want_kv=False)

    @pl.when(chip == 0)
    def _():
        sib_qd.wait_recv()
        sib_row.wait_recv()

    @pl.when(core == 1)
    def _():
        for i in range(NX):
            kv_x(i).wait_recv()
            part(queries(0), kvx, i * XCH, XCH, x_from * ROWS, dq_rows=everything, want_kv=False)

    @pl.when(core == 0)
    def _():
        pl.when(rank != 4)(lambda: sib_keys(0))
        sib_keys(XCH)

    @pl.when(far_right)
    def _():
        far_qd.wait_recv()
        far_row.wait_recv()
        far = [qfar[n].reshape(HEADS * XCH, DIM) for n in range(2)] + [rfar[1, n:n + 1, :] for n in range(3)]
        dk, dv = part(far, kvown, 0, XCH, rank * ROWS)
        own[0, 0:XCH] += dk
        own[1, 0:XCH] += dv

    @pl.when(rank == 0)
    def _():
        for i in range(NRLY):
            give_relay(i, LOFF[i], LSIZE[i]).wait_recv()
            pass_on(i, LOFF[i], LSIZE[i]).start()

    for g in range(HEADS):
        lanes = slice(g * ROWS, (g + 1) * ROWS)
        dq_ref[lanes] = (dqt[:, lanes].T * scale).astype(BF16)

    for i in range(NL):
        span = slice(LOFF[i], LOFF[i] + LSIZE[i])

        @pl.when(has_r)
        def _():
            give_left(i, LOFF[i], LSIZE[i]).wait_recv()
            own[:, span] += lret[:, span]

        if i == NL - 1:
            @pl.when(far_right)
            def _():
                give_x().wait_recv()
                own[:, XCH:] += xret[...]
            span = slice(XCH, ROWS)
        elif LOFF[i] >= XCH:
            continue
        dk_ref[span, :] = (own[0, span] * scale).astype(BF16)
        dv_ref[span, :] = own[1, span].astype(BF16)

    for i in range(NL):
        at = (i, LOFF[i], LSIZE[i])
        pl.when(has_r)(lambda: kv_right(*at).wait_send())

        @pl.when(has_l)
        def _():
            kv_relay(*at).wait_send()
            give_left(*at).wait_send()

        if i < NRLY:
            pl.when(rank == 0)(lambda: pass_on(*at).wait_send())
    for i in range(NX):
        pl.when(x_ret)(lambda: kv_x(i).wait_send())
    sib_qd.wait_send()
    sib_row.wait_send()

    pl.when(chip == 3)(lambda: bounce_on().wait_send())

    @pl.when(far_left)
    def _():
        far_qd.wait_send()
        far_row.wait_send()
        give_x().wait_send()


def write_out(dq_ref, dk_ref, dv_ref, dq_hbm, dk_hbm, dv_hbm, sem):
    copies = [pltpu.make_async_copy(src, dst, sem.at[n]) for n, (src, dst) in enumerate([
        (dq_ref, dq_hbm), (dk_ref, dk_hbm), (dv_ref, dv_hbm)])]
    for copy in copies:
        copy.start()
    for copy in copies:
        copy.wait()


def solution(mesh):
    def local(queries, keys, values, attn_out, logsumexp, d_out, cu_seqlens):
        rows, heads, head = queries.shape
        flat = lambda a: jnp.transpose(a, (1, 0, 2))
        kv = pltpu.VMEM((2, rows, head), BF16)
        sums = pltpu.VMEM((2, rows, head), F32)
        row = pltpu.VMEM((2, 8, QALL), F32)
        qd = pltpu.VMEM((2, 2, heads, rows, head), BF16)
        xsum = pltpu.VMEM((2, XCH, head), F32)
        dma = pltpu.SemaphoreType.DMA
        anyspec = pl.BlockSpec(memory_space=pl.ANY)
        vspec = pl.BlockSpec(memory_space=pltpu.VMEM)
        dq, dk, dv = pl.pallas_call(
            kernel,
            out_shape=(pltpu.VMEM((QALL, head), BF16), pltpu.VMEM((rows, head), BF16), pltpu.VMEM((rows, head), BF16)),
            in_specs=[anyspec] * 7,
            out_specs=(vspec, vspec, vspec),
            scratch_shapes=[pltpu.SMEM((NBOUND,), jnp.int32), qd, row, pltpu.VMEM((2, heads, XCH, head), BF16),
                            pltpu.VMEM((2, 8, heads * XCH), F32), pltpu.VMEM((heads, rows, head), BF16),
                            pltpu.VMEM((heads, rows), F32), kv, kv, pltpu.VMEM((2, 2, rows, head), BF16),
                            pltpu.VMEM((2, LSIZE[-1], head), BF16),
                            pltpu.VMEM((head, QALL), F32), sums, sums, xsum, sums, xsum, sums,
                            dma((7,)), dma((4,)), dma((4,))] + [dma((NL,))] * 8 + [dma((NX,))] * 6,
            compiler_params=pltpu.CompilerParams(collective_id=0, has_side_effects=True,
                                                 vmem_limit_bytes=48 << 20),
        )(*[pltpu.with_memory_space_constraint(a, pltpu.HBM) for a in (
            cu_seqlens, flat(queries), keys, values, flat(attn_out), logsumexp.T, flat(d_out))])
        dq, dk, dv = pl.pallas_call(
            write_out,
            out_shape=(jax.ShapeDtypeStruct(dq.shape, BF16), jax.ShapeDtypeStruct(dk.shape, BF16),
                       jax.ShapeDtypeStruct(dv.shape, BF16)),
            in_specs=[vspec] * 3,
            out_specs=(anyspec,) * 3,
            scratch_shapes=[dma((3,))],
            compiler_params=pltpu.CompilerParams(vmem_limit_bytes=4 << 20),
        )(dq, dk, dv)
        return jnp.transpose(dq.reshape(heads, rows, head), (1, 0, 2)), dk, dv

    seq = P(("dp", "cpo", "cp"))
    return jax.shard_map(local, mesh=mesh, in_specs=(seq,) * 6 + (P("dp"),), out_specs=(seq, seq, seq), check_vma=False)
```

```python
import math

import jax
import jax.numpy as jnp
from jax import lax
from jax.experimental import pallas as pl
from jax.experimental.pallas import tpu as pltpu
from jax.sharding import PartitionSpec as P

ROWS = 512
HEADS = 3
DIM = 128
NBOUND = 14
QALL = HEADS * ROWS
XCH = 256
NX = ROWS // XCH
PCH = 128
LSIZE = (64, 64, 128, 128, 128)
LOFF = (0, 64, 128, 256, 384)
NL = len(LSIZE)
NRLY = 5
STEPS = tuple(zip(LOFF, LSIZE))
LOG2E = math.log2(math.e)
MESH = pl.DeviceIdType.MESH
F32 = jnp.float32
BF16 = jnp.bfloat16
NT = (((1,), (1,)), ((), ()))
TN = (((0,), (0,)), ((), ()))


def device(rank):
    return (0, rank >> 2, rank & 3)


def kernel(cu_hbm, q_hbm, k_hbm, v_hbm, o_hbm, lse_hbm, do_hbm, dq_ref, dk_ref, dv_ref,
           cu_ref, qd, row, qfar, rfar, o_ref, lse_ref, kvown, kvx, kvl, kvb, dqt, own, mine, xout, lret, xret, rly,
           in_sem, sb_s, sb_r, kv_s, kv_r, re_s, re_r, le_s, le_r, ry_s, ry_r, kx_s, kx_r, xo_s, xo_r, bn_s, bn_r):
    rank = lax.axis_index("cpo") * 4 + lax.axis_index("cp")
    core = rank & 1
    chip = rank >> 1
    sib = rank + 1 - 2 * core
    scale = DIM ** -0.5

    loads = [pltpu.make_async_copy(src, dst, in_sem.at[n]) for n, (src, dst) in enumerate([
        (k_hbm, kvown.at[0]), (v_hbm, kvown.at[1]), (do_hbm, qd.at[0, 1]), (q_hbm, qd.at[0, 0]), (o_hbm, o_ref),
        (lse_hbm, lse_ref), (cu_hbm, cu_ref)])]
    loads[0].start()
    loads[1].start()

    has_l = chip >= 1
    has_r = chip <= 2
    x_from = jnp.where(core == 1, rank - 1, rank - 3)
    x_to = jnp.where(core == 1, rank + 3, rank + 1)
    has_x = x_from >= 0
    x_ret = x_to <= 7

    barrier = pltpu.get_barrier_semaphore()

    def greet(other):
        pl.semaphore_signal(barrier, inc=1, device_id=device(other), device_id_type=MESH)

    far_right = (core == 1) & (chip <= 1)
    far_left = (core == 0) & (chip >= 2)
    left = sib - 2
    right = sib + 2
    pl.when(has_l)(lambda: greet(left))
    pl.when(has_r)(lambda: greet(right))
    pl.when(far_right)(lambda: greet(rank + 3))
    pl.when(far_left)(lambda: greet(rank - 3))
    pl.when(chip == 1)(lambda: greet(rank + 4))
    pl.when(chip == 3)(lambda: greet(rank - 4))
    pl.when(rank == 1)(lambda: greet(5))
    pl.when(rank == 5)(lambda: greet(1))
    greet(sib)
    for copy in loads[2:]:
        copy.start()
    one = jnp.int32(1)
    zero = jnp.int32(0)
    count = one
    for there in (has_l, has_r, far_right, far_left, chip == 1, chip == 3, rank == 1, rank == 5):
        count = count + jnp.where(there, one, zero)
    pl.semaphore_wait(barrier, count)

    def remote(src, dst, s_sem, r_sem, other):
        return pltpu.make_async_remote_copy(src_ref=src, dst_ref=dst, send_sem=s_sem, recv_sem=r_sem,
                                            device_id=device(other), device_id_type=MESH)

    def rows(off, size):
        return pl.ds(off, size)

    def lend(src, dst, n, other):
        return remote(src, dst, sb_s.at[n], sb_r.at[n], other)

    def kv_right(i, off, size):
        return remote(kvown.at[:, rows(off, size)], kvl.at[core, :, rows(off, size)], kv_s.at[i], kv_r.at[i], right)

    def kv_in(i, off, size):
        return remote(kvown.at[:, rows(off, size)], kvl.at[1 - core, :, rows(off, size)], kv_s.at[i], kv_r.at[i], left)

    last = pl.ds(LOFF[-1], LSIZE[-1])

    def bounce():
        return remote(kvown.at[:, last], kvb, kv_s.at[NL - 1], bn_r.at[0], rank + 4)

    def bounce_on():
        return remote(kvb, kvl.at[core, :, last], bn_s.at[0], kv_r.at[NL - 1], left)

    def kv_relay(i, off, size):
        part = kvl.at[1 - core, :, rows(off, size)]
        return remote(part, part, re_s.at[i], re_r.at[i], sib)

    def kv_relayed(i, off, size):
        part = kvl.at[core, :, rows(off, size)]
        return remote(part, part, re_s.at[i], re_r.at[i], sib)

    def kv_x(i):
        return remote(kvown.at[:, rows(i * XCH, XCH)], kvx.at[:, rows(i * XCH, XCH)], kx_s.at[i], kx_r.at[i], x_to)

    def give_x(j):
        return remote(xout.at[:, rows(j * PCH, PCH)], xret.at[:, rows(j * PCH, PCH)], xo_s.at[j], xo_r.at[j], rank - 3)

    def give_left(i, off, size):
        return remote(mine.at[:, rows(off, size)], lret.at[:, rows(off, size)], le_s.at[i], le_r.at[i], left)

    def give_relay(i, off, size):
        return remote(mine.at[:, rows(off, size)], rly.at[:, rows(off, size)], le_s.at[i], ry_r.at[i], 1)

    def pass_on(i, off, size):
        return remote(rly.at[:, rows(off, size)], lret.at[:, rows(off, size)], ry_s.at[i], le_r.at[i], 2)

    loads[0].wait()
    loads[1].wait()

    @pl.when(has_r)
    def _():
        pl.when(chip == 1)(lambda: bounce().start())
        for i in range(NL - 1):
            kv_right(i, LOFF[i], LSIZE[i]).start()
        pl.when(chip != 1)(lambda: kv_right(NL - 1, LOFF[-1], LSIZE[-1]).start())

    loads[2].wait()
    loads[3].wait()
    sib_qd, sib_row = lend(qd.at[0], qd.at[1], 0, sib), lend(row.at[0], row.at[1], 1, sib)
    far_to = jnp.where(core == 0, rank - 3, rank + 3)
    far_qd, far_row = lend(qd.at[0, :, :, 0:XCH], qfar, 2, far_to), lend(rfar.at[0], rfar.at[1], 3, far_to)
    sib_qd.start()
    pl.when(far_left)(lambda: far_qd.start())

    pos = rank * ROWS + lax.broadcasted_iota(jnp.int32, (1, ROWS), 1)
    start = jnp.zeros((1, ROWS), jnp.int32)
    loads[6].wait()
    for n in range(NBOUND):
        bound = cu_ref[n]
        start = jnp.where(bound <= pos, bound, start)
    loads[4].wait()
    loads[5].wait()
    for g in range(HEADS):
        lanes = slice(g * ROWS, (g + 1) * ROWS)
        prod = qd[0, 1, g].astype(F32) * o_ref[g].astype(F32)
        half = slice(g * XCH, (g + 1) * XCH)
        for n, line in enumerate([lse_ref[g:g + 1, :] * LOG2E, jnp.sum(prod.T, axis=0, keepdims=True), start.astype(F32)]):
            row[0, n:n + 1, lanes] = line
            rfar[0, n:n + 1, half] = line[:, 0:XCH]
    sib_row.start()
    pl.when(far_left)(lambda: far_row.start())

    def lines(ref, spans):
        return [jnp.concatenate([ref[n:n + 1, span] for span in spans], axis=1) for n in range(3)]

    def queries(who):
        return [qd[who, n].reshape(QALL, DIM) for n in range(2)] + [row[who, n:n + 1, :] for n in range(3)]

    def own_rows(lo, hi):
        q, do = (qd[0, n, :, lo:hi].reshape(HEADS * (hi - lo), DIM) for n in range(2))
        return [q, do] + lines(row.at[0], [slice(g * ROWS + lo, g * ROWS + hi) for g in range(HEADS)])

    def part(query, kv, off, size, first_key, low=None, dq_rows=None, want_kv=True):
        q, do, lse, dot, start = query
        k = kv[0, off:off + size, :]
        v = kv[1, off:off + size, :]
        width = q.shape[0]
        key = lax.broadcasted_iota(jnp.int32, (size, width), 0)
        keep = (first_key + off + key).astype(F32) >= start
        if low is not None:
            keep = keep & (key <= lax.rem(lax.broadcasted_iota(jnp.int32, (size, width), 1), ROWS - low))
        s = lax.dot_general(k, q, NT, preferred_element_type=F32)
        dp = lax.dot_general(v, do, NT, preferred_element_type=F32)
        p = jnp.exp2(s * (scale * LOG2E) - lse)
        p = jnp.where(keep, p, 0.0)
        ds = (p * (dp - dot)).astype(BF16)
        if dq_rows is not None:
            lo, hi = dq_rows
            dq = lax.dot_general(k, ds, TN, preferred_element_type=F32)
            if low == 0:
                dqt[...] = dq
            elif hi - lo == ROWS:
                dqt[...] += dq
            else:
                for g in range(HEADS):
                    dqt[:, g * ROWS + lo:g * ROWS + hi] += dq[:, g * (hi - lo):(g + 1) * (hi - lo)]
        if want_kv:
            dv = jnp.dot(p.astype(BF16), do, preferred_element_type=F32)
            dk = jnp.dot(ds, q, preferred_element_type=F32)
            return dk, dv

    everything = (0, ROWS)

    for off in range(0, ROWS, XCH):
        dk, dv = part(own_rows(off, ROWS), kvown, off, XCH, rank * ROWS, low=off, dq_rows=(off, ROWS))
        own[0, off:off + XCH] = dk
        own[1, off:off + XCH] = dv

    pl.when(x_ret)(lambda: [kv_x(i).start() for i in range(NX)] and None)

    def lstep(n):
        off, size = STEPS[n]
        pieces = [(i, LOFF[i], LSIZE[i]) for i in range(NL) if off <= LOFF[i] < off + size]
        for piece in pieces:
            kv_in(*piece).wait_recv()
            kv_relay(*piece).start()
        mine_kv = kvl.at[1 - core]
        dk, dv = part(queries(0), mine_kv, off, size, left * ROWS, dq_rows=everything)
        if n == 0:
            @pl.when(rank != 4)
            def _():
                sib_qd.wait_recv()
                sib_row.wait_recv()
        dk2, dv2 = part(queries(1), mine_kv, off, size, left * ROWS)
        mine[0, off:off + size] = dk + dk2
        mine[1, off:off + size] = dv + dv2

        @pl.when(rank != 5)
        def _():
            for piece in pieces:
                give_left(*piece).start()

        @pl.when(rank == 5)
        def _():
            for piece in pieces:
                (give_relay if piece[0] < NRLY else give_left)(*piece).start()

    def sib_keys(off):
        dk, dv = part(queries(1), kvown, off, XCH, rank * ROWS)
        own[0, off:off + XCH] += dk
        own[1, off:off + XCH] += dv

    @pl.when(rank == 4)
    def _():
        sib_qd.wait_recv()
        sib_row.wait_recv()
        sib_keys(0)

    @pl.when(chip == 3)
    def _():
        bounce().wait_recv()
        bounce_on().start()

    @pl.when(has_l)
    def _():
        for n in range(len(STEPS)):
            lstep(n)

    @pl.when(far_left)
    def _():
        kv_x(1).wait_recv()
        dk, dv = part(queries(0), kvx, XCH, XCH, x_from * ROWS, dq_rows=everything)
        xout[0] = dk
        xout[1] = dv
        give_x(0).start()
        give_x(1).start()
        kv_x(0).wait_recv()
        part(own_rows(0, XCH), kvx, 0, XCH, x_from * ROWS, dq_rows=(0, XCH), want_kv=False)

    @pl.when(has_l)
    def _():
        for off in range(0, ROWS, XCH):
            for i in range(NL):
                if off <= LOFF[i] < off + XCH:
                    kv_relayed(i, LOFF[i], LSIZE[i]).wait_recv()
            part(queries(0), kvl.at[core], off, XCH, (rank - 2) * ROWS, dq_rows=everything, want_kv=False)

    @pl.when(chip == 0)
    def _():
        sib_qd.wait_recv()
        sib_row.wait_recv()

    @pl.when(core == 1)
    def _():
        for i in range(NX):
            kv_x(i).wait_recv()
            part(queries(0), kvx, i * XCH, XCH, x_from * ROWS, dq_rows=everything, want_kv=False)

    @pl.when(core == 0)
    def _():
        pl.when(rank != 4)(lambda: sib_keys(0))
        sib_keys(XCH)

    @pl.when(far_right)
    def _():
        far_qd.wait_recv()
        far_row.wait_recv()
        far = [qfar[n].reshape(HEADS * XCH, DIM) for n in range(2)] + [rfar[1, n:n + 1, :] for n in range(3)]
        dk, dv = part(far, kvown, 0, XCH, rank * ROWS)
        own[0, 0:XCH] += dk
        own[1, 0:XCH] += dv

    @pl.when(rank == 1)
    def _():
        for i in range(NRLY):
            give_relay(i, LOFF[i], LSIZE[i]).wait_recv()
            pass_on(i, LOFF[i], LSIZE[i]).start()

    for g in range(HEADS):
        lanes = slice(g * ROWS, (g + 1) * ROWS)
        dq_ref[lanes] = (dqt[:, lanes].T * scale).astype(BF16)

    for i in range(NL):
        at = (i, LOFF[i], LSIZE[i])
        pl.when(has_r)(lambda: kv_right(*at).wait_send())

        @pl.when(has_l)
        def _():
            kv_relay(*at).wait_send()
            give_left(*at).wait_send()

        if i < NRLY:
            pl.when(rank == 1)(lambda: pass_on(*at).wait_send())
    for i in range(NX):
        pl.when(x_ret)(lambda: kv_x(i).wait_send())
    sib_qd.wait_send()
    sib_row.wait_send()

    pl.when(chip == 3)(lambda: bounce_on().wait_send())

    @pl.when(far_left)
    def _():
        far_qd.wait_send()
        far_row.wait_send()
        give_x(0).wait_send()
        give_x(1).wait_send()

    for i in range(NL):
        span = slice(LOFF[i], LOFF[i] + LSIZE[i])

        @pl.when(has_r)
        def _():
            give_left(i, LOFF[i], LSIZE[i]).wait_recv()
            own[:, span] += lret[:, span]

        if LOFF[i] >= XCH:
            @pl.when(far_right)
            def _():
                give_x(i - NL + 2).wait_recv()
                own[:, span] += xret[:, LOFF[i] - XCH:LOFF[i] - XCH + LSIZE[i]]

        dk_ref[span, :] = (own[0, span] * scale).astype(BF16)
        dv_ref[span, :] = own[1, span].astype(BF16)


def write_out(dq_ref, dk_ref, dv_ref, dq_hbm, dk_hbm, dv_hbm, sem):
    copies = [pltpu.make_async_copy(src, dst, sem.at[n]) for n, (src, dst) in enumerate([
        (dq_ref, dq_hbm), (dk_ref, dk_hbm), (dv_ref, dv_hbm)])]
    for copy in copies:
        copy.start()
    for copy in copies:
        copy.wait()


def solution(mesh):
    def local(queries, keys, values, attn_out, logsumexp, d_out, cu_seqlens):
        rows, heads, head = queries.shape
        flat = lambda a: jnp.transpose(a, (1, 0, 2))
        kv = pltpu.VMEM((2, rows, head), BF16)
        sums = pltpu.VMEM((2, rows, head), F32)
        row = pltpu.VMEM((2, 8, QALL), F32)
        qd = pltpu.VMEM((2, 2, heads, rows, head), BF16)
        xsum = pltpu.VMEM((2, XCH, head), F32)
        dma = pltpu.SemaphoreType.DMA
        anyspec = pl.BlockSpec(memory_space=pl.ANY)
        vspec = pl.BlockSpec(memory_space=pltpu.VMEM)
        dq, dk, dv = pl.pallas_call(
            kernel,
            out_shape=(pltpu.VMEM((QALL, head), BF16), pltpu.VMEM((rows, head), BF16), pltpu.VMEM((rows, head), BF16)),
            in_specs=[anyspec] * 7,
            out_specs=(vspec, vspec, vspec),
            scratch_shapes=[pltpu.SMEM((NBOUND,), jnp.int32), qd, row, pltpu.VMEM((2, heads, XCH, head), BF16),
                            pltpu.VMEM((2, 8, heads * XCH), F32), pltpu.VMEM((heads, rows, head), BF16),
                            pltpu.VMEM((heads, rows), F32), kv, kv, pltpu.VMEM((2, 2, rows, head), BF16),
                            pltpu.VMEM((2, LSIZE[-1], head), BF16),
                            pltpu.VMEM((head, QALL), F32), sums, sums, xsum, sums, xsum, sums,
                            dma((7,)), dma((4,)), dma((4,))] + [dma((NL,))] * 8 + [dma((NX,))] * 6,
            compiler_params=pltpu.CompilerParams(collective_id=0, has_side_effects=True,
                                                 vmem_limit_bytes=48 << 20),
        )(*[pltpu.with_memory_space_constraint(a, pltpu.HBM) for a in (
            cu_seqlens, flat(queries), keys, values, flat(attn_out), logsumexp.T, flat(d_out))])
        dq, dk, dv = pl.pallas_call(
            write_out,
            out_shape=(jax.ShapeDtypeStruct(dq.shape, BF16), jax.ShapeDtypeStruct(dk.shape, BF16),
                       jax.ShapeDtypeStruct(dv.shape, BF16)),
            in_specs=[vspec] * 3,
            out_specs=(anyspec,) * 3,
            scratch_shapes=[dma((3,))],
            compiler_params=pltpu.CompilerParams(vmem_limit_bytes=4 << 20),
        )(dq, dk, dv)
        return jnp.transpose(dq.reshape(heads, rows, head), (1, 0, 2)), dk, dv

    seq = P(("dp", "cpo", "cp"))
    return jax.shard_map(local, mesh=mesh, in_specs=(seq,) * 6 + (P("dp"),), out_specs=(seq, seq, seq), check_vma=False)
```

```python
import math

import jax
import jax.numpy as jnp
from jax import lax
from jax.experimental import pallas as pl
from jax.experimental.pallas import tpu as pltpu
from jax.sharding import PartitionSpec as P

ROWS = 512
HEADS = 3
DIM = 128
NBOUND = 14
QALL = HEADS * ROWS
XCH = 256
NX = ROWS // XCH
PCH = 128
LSIZE = (64, 64, 128, 128, 128)
LOFF = (0, 64, 128, 256, 384)
NL = len(LSIZE)
NRLY = 5
STEPS = tuple(zip(LOFF, LSIZE))
LOG2E = math.log2(math.e)
MESH = pl.DeviceIdType.MESH
F32 = jnp.float32
BF16 = jnp.bfloat16
NT = (((1,), (1,)), ((), ()))
TN = (((0,), (0,)), ((), ()))


def device(rank):
    return (0, rank >> 2, rank & 3)


def kernel(cu_hbm, q_hbm, k_hbm, v_hbm, o_hbm, lse_hbm, do_hbm, dq_ref, dk_ref, dv_ref,
           cu_ref, qd, row, qfar, rfar, o_ref, lse_ref, kvown, kvx, kvl, kvb, dqt, own, mine, xout, lret, xret, rly,
           in_sem, out_sem, lend_r, kv_r, re_r, le_r, kx_r, xo_r):
    rank = lax.axis_index("cpo") * 4 + lax.axis_index("cp")
    core = rank & 1
    chip = rank >> 1
    sib = rank + 1 - 2 * core
    scale = DIM ** -0.5

    sems = (0, 0, 1, 1, 2, 3, 4)
    loads = [pltpu.make_async_copy(src, dst, in_sem.at[n]) for n, (src, dst) in zip(sems, [
        (k_hbm, kvown.at[0]), (v_hbm, kvown.at[1]), (do_hbm, qd.at[0, 1]), (q_hbm, qd.at[0, 0]), (o_hbm, o_ref),
        (lse_hbm, lse_ref), (cu_hbm, cu_ref)])]
    kv_loaded = pltpu.make_async_copy(kvown, kvown, in_sem.at[0])
    qd_loaded = pltpu.make_async_copy(qd.at[0], qd.at[0], in_sem.at[1])
    loads[0].start()
    loads[1].start()

    has_l = chip >= 1
    has_r = chip <= 2
    x_from = jnp.where(core == 1, rank - 1, rank - 3)
    x_to = jnp.where(core == 1, rank + 3, rank + 1)
    has_x = x_from >= 0
    x_ret = x_to <= 7

    barrier = pltpu.get_barrier_semaphore()

    def greet(other):
        pl.semaphore_signal(barrier, inc=1, device_id=device(other), device_id_type=MESH)

    far_right = (core == 1) & (chip <= 1)
    far_left = (core == 0) & (chip >= 2)
    left = sib - 2
    right = sib + 2
    pl.when(has_l)(lambda: greet(left))
    pl.when(has_r)(lambda: greet(right))
    pl.when(far_right)(lambda: greet(rank + 3))
    pl.when(far_left)(lambda: greet(rank - 3))
    pl.when(chip == 1)(lambda: greet(rank + 4))
    pl.when(chip == 3)(lambda: greet(rank - 4))
    pl.when(rank == 1)(lambda: greet(5))
    pl.when(rank == 5)(lambda: greet(1))
    greet(sib)
    for copy in loads[2:]:
        copy.start()
    one = jnp.int32(1)
    zero = jnp.int32(0)
    count = one
    for there in (has_l, has_r, far_right, far_left, chip == 1, chip == 3, rank == 1, rank == 5):
        count = count + jnp.where(there, one, zero)
    pl.semaphore_wait(barrier, count)

    def remote(src, dst, s_sem, r_sem, other):
        return pltpu.make_async_remote_copy(src_ref=src, dst_ref=dst, send_sem=s_sem, recv_sem=r_sem,
                                            device_id=device(other), device_id_type=MESH)

    def rows(off, size):
        return pl.ds(off, size)

    kv_s, kx_s, re_s, le_s, xo_s = in_sem.at[0], out_sem.at[0], out_sem.at[1], out_sem.at[2], out_sem.at[3]
    last = pl.ds(LOFF[-1], LSIZE[-1])
    whole = (NL, 0, ROWS)
    halves = ((0, 0, XCH), (NL - 1, XCH, XCH))

    def half_of(i):
        return min(i // 3, 1)

    def third(i):
        return min(max(i - 2, 0), 2)

    def lend(src, dst, s_n, r_n, other):
        return remote(src, dst, in_sem.at[s_n], lend_r.at[r_n], other)

    def kv_right(i, off, size):
        return remote(kvown.at[:, rows(off, size)], kvl.at[core, :, rows(off, size)], kv_s, kv_r.at[min(i, NL - 1)], right)

    def kv_in(i, off, size):
        return remote(kvown.at[:, rows(off, size)], kvl.at[1 - core, :, rows(off, size)], kv_s, kv_r.at[i], left)

    def bounce():
        return remote(kvown.at[:, last], kvb, kv_s, le_r.at[0], rank + 4)

    def bounce_on():
        return remote(kvb, kvl.at[core, :, last], kv_s, kv_r.at[NL - 1], left)

    def kv_relay(i, off, size):
        part = kvl.at[1 - core, :, rows(off, size)]
        return remote(part, part, re_s, re_r.at[half_of(i)], sib)

    def kv_relayed(i, off, size):
        part = kvl.at[core, :, rows(off, size)]
        return remote(part, part, re_s, re_r.at[half_of(i)], sib)

    def kv_x():
        return remote(kvown, kvx, kx_s, kx_r.at[0], x_to)

    def give_x():
        return remote(xout, xret, xo_s, xo_r.at[0], rank - 3)

    def give_left(i, off, size):
        return remote(mine.at[:, rows(off, size)], lret.at[:, rows(off, size)], le_s, le_r.at[third(i)], left)

    def give_relay(i, off, size):
        return remote(mine.at[:, rows(off, size)], rly.at[:, rows(off, size)], le_s, kv_r.at[i], 1)

    def pass_on(i, off, size):
        return remote(rly.at[:, rows(off, size)], lret.at[:, rows(off, size)], le_s, le_r.at[third(i)], 2)

    kv_loaded.wait()

    @pl.when(has_r)
    def _():
        pl.when(chip == 1)(lambda: bounce().start())
        for i in range(NL - 1):
            kv_right(i, LOFF[i], LSIZE[i]).start()
        pl.when(chip != 1)(lambda: kv_right(NL - 1, LOFF[-1], LSIZE[-1]).start())

    qd_loaded.wait()
    far_to = jnp.where(core == 0, rank - 3, rank + 3)
    sib_qd, sib_row = lend(qd.at[0], qd.at[1], 1, 0, sib), lend(row.at[0], row.at[1], 3, 1, sib)
    far_qd, far_row = lend(qd.at[0, :, :, 0:XCH], qfar, 4, 2, far_to), lend(rfar.at[0], rfar.at[1], 2, 3, far_to)
    loads[6].wait()
    pl.when(far_left)(lambda: far_qd.start())
    sib_qd.start()

    pos = rank * ROWS + lax.broadcasted_iota(jnp.int32, (1, ROWS), 1)
    start = jnp.zeros((1, ROWS), jnp.int32)
    for n in range(NBOUND):
        bound = cu_ref[n]
        start = jnp.where(bound <= pos, bound, start)
    loads[4].wait()
    loads[5].wait()
    for g in range(HEADS):
        lanes = slice(g * ROWS, (g + 1) * ROWS)
        prod = qd[0, 1, g].astype(F32) * o_ref[g].astype(F32)
        half = slice(g * XCH, (g + 1) * XCH)
        for n, line in enumerate([lse_ref[g:g + 1, :] * LOG2E, jnp.sum(prod.T, axis=0, keepdims=True), start.astype(F32)]):
            row[0, n:n + 1, lanes] = line
            rfar[0, n:n + 1, half] = line[:, 0:XCH]
    sib_row.start()
    pl.when(far_left)(lambda: far_row.start())

    def lines(ref, spans):
        return [jnp.concatenate([ref[n:n + 1, span] for span in spans], axis=1) for n in range(3)]

    def queries(who):
        return [qd[who, n].reshape(QALL, DIM) for n in range(2)] + [row[who, n:n + 1, :] for n in range(3)]

    def own_rows(lo, hi):
        q, do = (qd[0, n, :, lo:hi].reshape(HEADS * (hi - lo), DIM) for n in range(2))
        return [q, do] + lines(row.at[0], [slice(g * ROWS + lo, g * ROWS + hi) for g in range(HEADS)])

    def part(query, kv, off, size, first_key, low=None, dq_rows=None, want_kv=True):
        q, do, lse, dot, start = query
        k = kv[0, off:off + size, :]
        v = kv[1, off:off + size, :]
        width = q.shape[0]
        key = lax.broadcasted_iota(jnp.int32, (size, width), 0)
        keep = (first_key + off + key).astype(F32) >= start
        if low is not None:
            keep = keep & (key <= lax.rem(lax.broadcasted_iota(jnp.int32, (size, width), 1), ROWS - low))
        s = lax.dot_general(k, q, NT, preferred_element_type=F32)
        dp = lax.dot_general(v, do, NT, preferred_element_type=F32)
        p = jnp.exp2(s * (scale * LOG2E) - lse)
        p = jnp.where(keep, p, 0.0)
        ds = (p * (dp - dot)).astype(BF16)
        if dq_rows is not None:
            lo, hi = dq_rows
            dq = lax.dot_general(k, ds, TN, preferred_element_type=F32)
            if low == 0:
                dqt[...] = dq
            elif hi - lo == ROWS:
                dqt[...] += dq
            else:
                for g in range(HEADS):
                    dqt[:, g * ROWS + lo:g * ROWS + hi] += dq[:, g * (hi - lo):(g + 1) * (hi - lo)]
        if want_kv:
            dv = jnp.dot(p.astype(BF16), do, preferred_element_type=F32)
            dk = jnp.dot(ds, q, preferred_element_type=F32)
            return dk, dv

    everything = (0, ROWS)

    for off in range(0, ROWS, XCH):
        dk, dv = part(own_rows(off, ROWS), kvown, off, XCH, rank * ROWS, low=off, dq_rows=(off, ROWS))
        own[0, off:off + XCH] = dk
        own[1, off:off + XCH] = dv

    pl.when(x_ret)(lambda: kv_x().start())

    def lstep(n):
        off, size = STEPS[n]
        pieces = [(i, LOFF[i], LSIZE[i]) for i in range(NL) if off <= LOFF[i] < off + size]
        for piece in pieces:
            kv_in(*piece).wait_recv()
            kv_relay(*piece).start()
        mine_kv = kvl.at[1 - core]
        dk, dv = part(queries(0), mine_kv, off, size, left * ROWS, dq_rows=everything)
        if n == 0:
            @pl.when(rank != 4)
            def _():
                sib_qd.wait_recv()
                sib_row.wait_recv()
        dk2, dv2 = part(queries(1), mine_kv, off, size, left * ROWS)
        mine[0, off:off + size] = dk + dk2
        mine[1, off:off + size] = dv + dv2

        @pl.when(rank != 5)
        def _():
            for piece in pieces:
                give_left(*piece).start()

        @pl.when(rank == 5)
        def _():
            for piece in pieces:
                (give_relay if piece[0] < NRLY else give_left)(*piece).start()

    def sib_keys(off):
        dk, dv = part(queries(1), kvown, off, XCH, rank * ROWS)
        own[0, off:off + XCH] += dk
        own[1, off:off + XCH] += dv

    @pl.when(rank == 4)
    def _():
        sib_qd.wait_recv()
        sib_row.wait_recv()
        sib_keys(0)

    @pl.when(chip == 3)
    def _():
        bounce().wait_recv()
        bounce_on().start()

    @pl.when(has_l)
    def _():
        for n in range(len(STEPS)):
            lstep(n)

    @pl.when(far_left)
    def _():
        kv_x().wait_recv()
        dk, dv = part(queries(0), kvx, XCH, XCH, x_from * ROWS, dq_rows=everything)
        xout[0] = dk
        xout[1] = dv
        give_x().start()
        part(own_rows(0, XCH), kvx, 0, XCH, x_from * ROWS, dq_rows=(0, XCH), want_kv=False)

    @pl.when(has_l)
    def _():
        for off in range(0, ROWS, XCH):
            kv_relayed(*halves[off // XCH]).wait_recv()
            part(queries(0), kvl.at[core], off, XCH, (rank - 2) * ROWS, dq_rows=everything, want_kv=False)

    @pl.when(chip == 0)
    def _():
        sib_qd.wait_recv()
        sib_row.wait_recv()

    @pl.when(core == 1)
    def _():
        kv_x().wait_recv()
        for i in range(NX):
            part(queries(0), kvx, i * XCH, XCH, x_from * ROWS, dq_rows=everything, want_kv=False)

    @pl.when(core == 0)
    def _():
        pl.when(rank != 4)(lambda: sib_keys(0))
        sib_keys(XCH)

    @pl.when(far_right)
    def _():
        far_qd.wait_recv()
        far_row.wait_recv()
        far = [qfar[n].reshape(HEADS * XCH, DIM) for n in range(2)] + [rfar[1, n:n + 1, :] for n in range(3)]
        dk, dv = part(far, kvown, 0, XCH, rank * ROWS)
        own[0, 0:XCH] += dk
        own[1, 0:XCH] += dv

    @pl.when(rank == 1)
    def _():
        for i in range(NRLY):
            give_relay(i, LOFF[i], LSIZE[i]).wait_recv()
            pass_on(i, LOFF[i], LSIZE[i]).start()

    for g in range(HEADS):
        lanes = slice(g * ROWS, (g + 1) * ROWS)
        dq_ref[lanes] = (dqt[:, lanes].T * scale).astype(BF16)

    pl.when(has_r)(lambda: kv_right(*whole).wait_send())
    pl.when(chip == 3)(lambda: bounce_on().wait_send())
    pl.when(x_ret)(lambda: kv_x().wait_send())
    sib_qd.wait_send()
    sib_row.wait_send()

    @pl.when(far_left)
    def _():
        far_qd.wait_send()
        far_row.wait_send()
        give_x().wait_send()

    @pl.when(has_l)
    def _():
        kv_relay(*whole).wait_send()
        give_left(*whole).wait_send()

    pl.when(rank == 1)(lambda: pass_on(*whole).wait_send())

    for i, off, size in ((0, 0, XCH), (3, LOFF[3], LSIZE[3]), (4, LOFF[4], LSIZE[4])):
        span = slice(off, off + size)

        @pl.when(has_r)
        def _():
            give_left(i, off, size).wait_recv()
            own[:, span] += lret[:, span]

        if off == XCH:
            @pl.when(far_right)
            def _():
                give_x().wait_recv()
                own[:, XCH:] += xret[...]

        dk_ref[span, :] = (own[0, span] * scale).astype(BF16)
        dv_ref[span, :] = own[1, span].astype(BF16)


def write_out(dq_ref, dk_ref, dv_ref, dq_hbm, dk_hbm, dv_hbm, sem):
    copies = [pltpu.make_async_copy(src, dst, sem.at[n]) for n, (src, dst) in enumerate([
        (dq_ref, dq_hbm), (dk_ref, dk_hbm), (dv_ref, dv_hbm)])]
    for copy in copies:
        copy.start()
    for copy in copies:
        copy.wait()


def solution(mesh):
    def local(queries, keys, values, attn_out, logsumexp, d_out, cu_seqlens):
        rows, heads, head = queries.shape
        flat = lambda a: jnp.transpose(a, (1, 0, 2))
        kv = pltpu.VMEM((2, rows, head), BF16)
        sums = pltpu.VMEM((2, rows, head), F32)
        row = pltpu.VMEM((2, 8, QALL), F32)
        qd = pltpu.VMEM((2, 2, heads, rows, head), BF16)
        xsum = pltpu.VMEM((2, XCH, head), F32)
        dma = pltpu.SemaphoreType.DMA
        anyspec = pl.BlockSpec(memory_space=pl.ANY)
        vspec = pl.BlockSpec(memory_space=pltpu.VMEM)
        dq, dk, dv = pl.pallas_call(
            kernel,
            out_shape=(pltpu.VMEM((QALL, head), BF16), pltpu.VMEM((rows, head), BF16), pltpu.VMEM((rows, head), BF16)),
            in_specs=[anyspec] * 7,
            out_specs=(vspec, vspec, vspec),
            scratch_shapes=[pltpu.SMEM((NBOUND,), jnp.int32), qd, row, pltpu.VMEM((2, heads, XCH, head), BF16),
                            pltpu.VMEM((2, 8, heads * XCH), F32), pltpu.VMEM((heads, rows, head), BF16),
                            pltpu.VMEM((heads, rows), F32), kv, kv, pltpu.VMEM((2, 2, rows, head), BF16),
                            pltpu.VMEM((2, LSIZE[-1], head), BF16),
                            pltpu.VMEM((head, QALL), F32), sums, sums, xsum, sums, xsum, sums,
                            dma((5,)), dma((4,)), dma((4,)), dma((NL,)), dma((2,)), dma((3,)), dma((1,)), dma((1,))],
            compiler_params=pltpu.CompilerParams(collective_id=0, has_side_effects=True,
                                                 vmem_limit_bytes=48 << 20),
        )(*[pltpu.with_memory_space_constraint(a, pltpu.HBM) for a in (
            cu_seqlens, flat(queries), keys, values, flat(attn_out), logsumexp.T, flat(d_out))])
        dq, dk, dv = pl.pallas_call(
            write_out,
            out_shape=(jax.ShapeDtypeStruct(dq.shape, BF16), jax.ShapeDtypeStruct(dk.shape, BF16),
                       jax.ShapeDtypeStruct(dv.shape, BF16)),
            in_specs=[vspec] * 3,
            out_specs=(anyspec,) * 3,
            scratch_shapes=[dma((3,))],
            compiler_params=pltpu.CompilerParams(vmem_limit_bytes=4 << 20),
        )(dq, dk, dv)
        return jnp.transpose(dq.reshape(heads, rows, head), (1, 0, 2)), dk, dv

    seq = P(("dp", "cpo", "cp"))
    return jax.shard_map(local, mesh=mesh, in_specs=(seq,) * 6 + (P("dp"),), out_specs=(seq, seq, seq), check_vma=False)
```

```python
import math

import jax
import jax.numpy as jnp
from jax import lax
from jax.experimental import pallas as pl
from jax.experimental.pallas import tpu as pltpu
from jax.sharding import PartitionSpec as P

ROWS = 512
HEADS = 3
DIM = 128
NBOUND = 14
QALL = HEADS * ROWS
XCH = 256
NX = ROWS // XCH
PCH = 128
LSIZE = (64, 64, 128, 96, 160)
LOFF = (0, 64, 128, 256, 352)
NL = len(LSIZE)
NRLY = 4
STEPS = tuple(zip(LOFF, LSIZE))
RLYROWS = sum(LSIZE[:NRLY])
LOG2E = math.log2(math.e)
MESH = pl.DeviceIdType.MESH
F32 = jnp.float32
BF16 = jnp.bfloat16
NT = (((1,), (1,)), ((), ()))
TN = (((0,), (0,)), ((), ()))


def device(rank):
    return (0, rank >> 2, rank & 3)


def kernel(cu_hbm, q_hbm, k_hbm, v_hbm, o_hbm, lse_hbm, do_hbm, dq_ref, dk_ref, dv_ref,
           cu_ref, qd, row, qfar, rfar, o_ref, lse_ref, kvown, kvx, kvl, kvb, dqt, own, mine, xout, lret, xret, rly,
           in_sem, out_sem, lend_r, kv_r, re_r, le_r, kx_r, xo_r):
    rank = lax.axis_index("cpo") * 4 + lax.axis_index("cp")
    core = rank & 1
    chip = rank >> 1
    sib = rank + 1 - 2 * core
    scale = DIM ** -0.5

    sems = (0, 0, 1, 1, 2, 3, 4)
    loads = [pltpu.make_async_copy(src, dst, in_sem.at[n]) for n, (src, dst) in zip(sems, [
        (k_hbm, kvown.at[0]), (v_hbm, kvown.at[1]), (do_hbm, qd.at[0, 1]), (q_hbm, qd.at[0, 0]), (o_hbm, o_ref),
        (lse_hbm, lse_ref), (cu_hbm, cu_ref)])]
    kv_loaded = pltpu.make_async_copy(kvown, kvown, in_sem.at[0])
    qd_loaded = pltpu.make_async_copy(qd.at[0], qd.at[0], in_sem.at[1])
    loads[0].start()
    loads[1].start()

    has_l = chip >= 1
    has_r = chip <= 2
    x_from = jnp.where(core == 1, rank - 1, rank - 3)
    x_to = jnp.where(core == 1, rank + 3, rank + 1)
    has_x = x_from >= 0
    x_ret = x_to <= 7

    barrier = pltpu.get_barrier_semaphore()

    def greet(other):
        pl.semaphore_signal(barrier, inc=1, device_id=device(other), device_id_type=MESH)

    far_right = (core == 1) & (chip <= 1)
    far_left = (core == 0) & (chip >= 2)
    left = sib - 2
    right = sib + 2
    pl.when(has_l)(lambda: greet(left))
    pl.when(has_r)(lambda: greet(right))
    pl.when(far_right)(lambda: greet(rank + 3))
    pl.when(far_left)(lambda: greet(rank - 3))
    pl.when(chip == 1)(lambda: greet(rank + 4))
    pl.when(chip == 3)(lambda: greet(rank - 4))
    pl.when(rank == 1)(lambda: greet(5))
    pl.when(rank == 5)(lambda: greet(1))
    greet(sib)
    for copy in loads[2:]:
        copy.start()
    one = jnp.int32(1)
    zero = jnp.int32(0)
    count = one
    for there in (has_l, has_r, far_right, far_left, chip == 1, chip == 3, rank == 1, rank == 5):
        count = count + jnp.where(there, one, zero)
    pl.semaphore_wait(barrier, count)

    def remote(src, dst, s_sem, r_sem, other):
        return pltpu.make_async_remote_copy(src_ref=src, dst_ref=dst, send_sem=s_sem, recv_sem=r_sem,
                                            device_id=device(other), device_id_type=MESH)

    def rows(off, size):
        return pl.ds(off, size)

    kv_s, kx_s, re_s, le_s, xo_s = in_sem.at[0], out_sem.at[0], out_sem.at[1], out_sem.at[2], out_sem.at[3]
    last = pl.ds(LOFF[-1], LSIZE[-1])
    whole = (NL, 0, ROWS)
    halves = ((0, 0, XCH), (NL - 1, XCH, XCH))

    def half_of(i):
        return min(i // 3, 1)

    def third(i):
        return min(max(i - 2, 0), 2)

    def lend(src, dst, s_n, r_n, other):
        return remote(src, dst, in_sem.at[s_n], lend_r.at[r_n], other)

    def kv_right(i, off, size):
        return remote(kvown.at[:, rows(off, size)], kvl.at[core, :, rows(off, size)], kv_s, kv_r.at[min(i, NL - 1)], right)

    def kv_in(i, off, size):
        return remote(kvown.at[:, rows(off, size)], kvl.at[1 - core, :, rows(off, size)], kv_s, kv_r.at[i], left)

    def bounce():
        return remote(kvown.at[:, last], kvb, kv_s, le_r.at[0], rank + 4)

    def bounce_on():
        return remote(kvb, kvl.at[core, :, last], kv_s, kv_r.at[NL - 1], left)

    def kv_relay(i, off, size):
        part = kvl.at[1 - core, :, rows(off, size)]
        return remote(part, part, re_s, re_r.at[half_of(i)], sib)

    def kv_relayed(i, off, size):
        part = kvl.at[core, :, rows(off, size)]
        return remote(part, part, re_s, re_r.at[half_of(i)], sib)

    def kv_x():
        return remote(kvown, kvx, kx_s, kx_r.at[0], x_to)

    def give_x():
        return remote(xout, xret, xo_s, xo_r.at[0], rank - 3)

    def give_left(i, off, size):
        return remote(mine.at[:, rows(off, size)], lret.at[:, rows(off, size)], le_s, le_r.at[third(i)], left)

    def give_relay(i, off, size):
        return remote(mine.at[:, rows(off, size)], rly.at[:, rows(off, size)], le_s, kv_r.at[i], 1)

    def pass_on(i, off, size):
        return remote(rly.at[:, rows(off, size)], lret.at[:, rows(off, size)], le_s, le_r.at[third(i)], 2)

    kv_loaded.wait()

    @pl.when(has_r)
    def _():
        pl.when(chip == 1)(lambda: bounce().start())
        for i in range(NL - 1):
            kv_right(i, LOFF[i], LSIZE[i]).start()
        pl.when(chip != 1)(lambda: kv_right(NL - 1, LOFF[-1], LSIZE[-1]).start())

    qd_loaded.wait()
    far_to = jnp.where(core == 0, rank - 3, rank + 3)
    sib_qd, sib_row = lend(qd.at[0], qd.at[1], 1, 0, sib), lend(row.at[0], row.at[1], 3, 1, sib)
    far_qd, far_row = lend(qd.at[0, :, :, 0:XCH], qfar, 4, 2, far_to), lend(rfar.at[0], rfar.at[1], 2, 3, far_to)
    loads[6].wait()
    pl.when(far_left)(lambda: far_qd.start())
    sib_qd.start()

    pos = rank * ROWS + lax.broadcasted_iota(jnp.int32, (1, ROWS), 1)
    start = jnp.zeros((1, ROWS), jnp.int32)
    for n in range(NBOUND):
        bound = cu_ref[n]
        start = jnp.where(bound <= pos, bound, start)
    loads[4].wait()
    loads[5].wait()
    for g in range(HEADS):
        lanes = slice(g * ROWS, (g + 1) * ROWS)
        prod = qd[0, 1, g].astype(F32) * o_ref[g].astype(F32)
        half = slice(g * XCH, (g + 1) * XCH)
        for n, line in enumerate([lse_ref[g:g + 1, :] * LOG2E, jnp.sum(prod.T, axis=0, keepdims=True), start.astype(F32)]):
            row[0, n:n + 1, lanes] = line
            rfar[0, n:n + 1, half] = line[:, 0:XCH]
    sib_row.start()
    pl.when(far_left)(lambda: far_row.start())

    def lines(ref, spans):
        return [jnp.concatenate([ref[n:n + 1, span] for span in spans], axis=1) for n in range(3)]

    def queries(who):
        return [qd[who, n].reshape(QALL, DIM) for n in range(2)] + [row[who, n:n + 1, :] for n in range(3)]

    def own_rows(lo, hi):
        q, do = (qd[0, n, :, lo:hi].reshape(HEADS * (hi - lo), DIM) for n in range(2))
        return [q, do] + lines(row.at[0], [slice(g * ROWS + lo, g * ROWS + hi) for g in range(HEADS)])

    def part(query, kv, off, size, first_key, low=None, dq_rows=None, want_kv=True):
        q, do, lse, dot, start = query
        k = kv[0, off:off + size, :]
        v = kv[1, off:off + size, :]
        width = q.shape[0]
        key = lax.broadcasted_iota(jnp.int32, (size, width), 0)
        keep = (first_key + off + key).astype(F32) >= start
        if low is not None:
            keep = keep & (key <= lax.rem(lax.broadcasted_iota(jnp.int32, (size, width), 1), ROWS - low))
        s = lax.dot_general(k, q, NT, preferred_element_type=F32)
        dp = lax.dot_general(v, do, NT, preferred_element_type=F32)
        p = jnp.exp2(s * (scale * LOG2E) - lse)
        p = jnp.where(keep, p, 0.0)
        ds = (p * (dp - dot)).astype(BF16)
        if dq_rows is not None:
            lo, hi = dq_rows
            dq = lax.dot_general(k, ds, TN, preferred_element_type=F32)
            if low == 0:
                dqt[...] = dq
            elif hi - lo == ROWS:
                dqt[...] += dq
            else:
                for g in range(HEADS):
                    dqt[:, g * ROWS + lo:g * ROWS + hi] += dq[:, g * (hi - lo):(g + 1) * (hi - lo)]
        if want_kv:
            dv = jnp.dot(p.astype(BF16), do, preferred_element_type=F32)
            dk = jnp.dot(ds, q, preferred_element_type=F32)
            return dk, dv

    everything = (0, ROWS)

    for off in range(0, ROWS, XCH):
        dk, dv = part(own_rows(off, ROWS), kvown, off, XCH, rank * ROWS, low=off, dq_rows=(off, ROWS))
        own[0, off:off + XCH] = dk
        own[1, off:off + XCH] = dv

    pl.when(x_ret)(lambda: kv_x().start())

    def fetch(n):
        kv_in(n, *STEPS[n]).wait_recv()
        kv_relay(n, *STEPS[n]).start()

    def lstep(n, fetched=False):
        off, size = STEPS[n]
        pieces = [(n, off, size)]
        if not fetched:
            fetch(n)
        mine_kv = kvl.at[1 - core]
        dk, dv = part(queries(0), mine_kv, off, size, left * ROWS, dq_rows=everything)
        if n == 0:
            @pl.when(rank != 4)
            def _():
                sib_qd.wait_recv()
                sib_row.wait_recv()
        dk2, dv2 = part(queries(1), mine_kv, off, size, left * ROWS)
        mine[0, off:off + size] = dk + dk2
        mine[1, off:off + size] = dv + dv2

        @pl.when(rank != 5)
        def _():
            for piece in pieces:
                give_left(*piece).start()

        if n < NRLY:
            pl.when(rank == 5)(lambda: give_relay(*pieces[0]).start())
        else:
            pl.when(rank == 5)(lambda: give_left(*pieces[0]).start())

    def sib_keys(off):
        dk, dv = part(queries(1), kvown, off, XCH, rank * ROWS)
        own[0, off:off + XCH] += dk
        own[1, off:off + XCH] += dv

    @pl.when(rank == 4)
    def _():
        sib_qd.wait_recv()
        sib_row.wait_recv()
        sib_keys(0)

    @pl.when(chip == 3)
    def _():
        bounce().wait_recv()
        bounce_on().start()

    @pl.when(has_l)
    def _():
        for n in range(NL - 2):
            lstep(n)
        pl.when(rank != 2)(lambda: lstep(NL - 2))

        @pl.when(rank == 2)
        def _():
            fetch(NL - 2)
            fetch(NL - 1)

    @pl.when(far_left)
    def _():
        kv_x().wait_recv()
        dk, dv = part(queries(0), kvx, XCH, XCH, x_from * ROWS, dq_rows=everything)
        xout[0] = dk
        xout[1] = dv
        give_x().start()

    pl.when(has_l & (rank != 2))(lambda: lstep(NL - 1))

    @pl.when(far_left)
    def _():
        part(own_rows(0, XCH), kvx, 0, XCH, x_from * ROWS, dq_rows=(0, XCH), want_kv=False)

    @pl.when(has_l)
    def _():
        for off in range(0, ROWS, XCH):
            kv_relayed(*halves[off // XCH]).wait_recv()
            part(queries(0), kvl.at[core], off, XCH, (rank - 2) * ROWS, dq_rows=everything, want_kv=False)

    @pl.when(chip == 0)
    def _():
        sib_qd.wait_recv()
        sib_row.wait_recv()

    @pl.when(core == 1)
    def _():
        kv_x().wait_recv()
        for i in range(NX):
            part(queries(0), kvx, i * XCH, XCH, x_from * ROWS, dq_rows=everything, want_kv=False)

    @pl.when(core == 0)
    def _():
        pl.when(rank != 4)(lambda: sib_keys(0))

        @pl.when(rank == 2)
        def _():
            lstep(NL - 2, fetched=True)
            lstep(NL - 1, fetched=True)

        sib_keys(XCH)

    @pl.when(far_right)
    def _():
        far_qd.wait_recv()
        far_row.wait_recv()
        far = [qfar[n].reshape(HEADS * XCH, DIM) for n in range(2)] + [rfar[1, n:n + 1, :] for n in range(3)]
        dk, dv = part(far, kvown, 0, XCH, rank * ROWS)
        own[0, 0:XCH] += dk
        own[1, 0:XCH] += dv

    @pl.when(rank == 1)
    def _():
        for i in range(NRLY):
            give_relay(i, LOFF[i], LSIZE[i]).wait_recv()
            pass_on(i, LOFF[i], LSIZE[i]).start()

    for g in range(HEADS):
        lanes = slice(g * ROWS, (g + 1) * ROWS)
        dq_ref[lanes] = (dqt[:, lanes].T * scale).astype(BF16)

    pl.when(has_r)(lambda: kv_right(*whole).wait_send())
    pl.when(chip == 3)(lambda: bounce_on().wait_send())
    pl.when(x_ret)(lambda: kv_x().wait_send())
    sib_qd.wait_send()
    sib_row.wait_send()

    @pl.when(far_left)
    def _():
        far_qd.wait_send()
        far_row.wait_send()
        give_x().wait_send()

    @pl.when(has_l)
    def _():
        kv_relay(*whole).wait_send()
        give_left(*whole).wait_send()

    pl.when(rank == 1)(lambda: pass_on(NL, 0, RLYROWS).wait_send())

    for i, off, size in ((0, 0, XCH), (3, LOFF[3], LSIZE[3]), (4, LOFF[4], LSIZE[4])):
        span = slice(off, off + size)

        if off == XCH:
            @pl.when(far_right)
            def _():
                give_x().wait_recv()
                own[:, XCH:] += xret[...]

        @pl.when(has_r)
        def _():
            give_left(i, off, size).wait_recv()
            dk_ref[span, :] = ((own[0, span] + lret[0, span]) * scale).astype(BF16)
            dv_ref[span, :] = (own[1, span] + lret[1, span]).astype(BF16)

        @pl.when(chip == 3)
        def _():
            dk_ref[span, :] = (own[0, span] * scale).astype(BF16)
            dv_ref[span, :] = own[1, span].astype(BF16)


def write_out(dq_ref, dk_ref, dv_ref, dq_hbm, dk_hbm, dv_hbm, sem):
    copies = [pltpu.make_async_copy(src, dst, sem.at[n]) for n, (src, dst) in enumerate([
        (dq_ref, dq_hbm), (dk_ref, dk_hbm), (dv_ref, dv_hbm)])]
    for copy in copies:
        copy.start()
    for copy in copies:
        copy.wait()


def solution(mesh):
    def local(queries, keys, values, attn_out, logsumexp, d_out, cu_seqlens):
        rows, heads, head = queries.shape
        flat = lambda a: jnp.transpose(a, (1, 0, 2))
        kv = pltpu.VMEM((2, rows, head), BF16)
        sums = pltpu.VMEM((2, rows, head), F32)
        row = pltpu.VMEM((2, 8, QALL), F32)
        qd = pltpu.VMEM((2, 2, heads, rows, head), BF16)
        xsum = pltpu.VMEM((2, XCH, head), F32)
        dma = pltpu.SemaphoreType.DMA
        anyspec = pl.BlockSpec(memory_space=pl.ANY)
        vspec = pl.BlockSpec(memory_space=pltpu.VMEM)
        dq, dk, dv = pl.pallas_call(
            kernel,
            out_shape=(pltpu.VMEM((QALL, head), BF16), pltpu.VMEM((rows, head), BF16), pltpu.VMEM((rows, head), BF16)),
            in_specs=[anyspec] * 7,
            out_specs=(vspec, vspec, vspec),
            scratch_shapes=[pltpu.SMEM((NBOUND,), jnp.int32), qd, row, pltpu.VMEM((2, heads, XCH, head), BF16),
                            pltpu.VMEM((2, 8, heads * XCH), F32), pltpu.VMEM((heads, rows, head), BF16),
                            pltpu.VMEM((heads, rows), F32), kv, kv, pltpu.VMEM((2, 2, rows, head), BF16),
                            pltpu.VMEM((2, LSIZE[-1], head), BF16),
                            pltpu.VMEM((head, QALL), F32), sums, sums, xsum, sums, xsum, sums,
                            dma((5,)), dma((4,)), dma((4,)), dma((NL,)), dma((2,)), dma((3,)), dma((1,)), dma((1,))],
            compiler_params=pltpu.CompilerParams(collective_id=0, has_side_effects=True,
                                                 vmem_limit_bytes=48 << 20),
        )(*[pltpu.with_memory_space_constraint(a, pltpu.HBM) for a in (
            cu_seqlens, flat(queries), keys, values, flat(attn_out), logsumexp.T, flat(d_out))])
        dq, dk, dv = pl.pallas_call(
            write_out,
            out_shape=(jax.ShapeDtypeStruct(dq.shape, BF16), jax.ShapeDtypeStruct(dk.shape, BF16),
                       jax.ShapeDtypeStruct(dv.shape, BF16)),
            in_specs=[vspec] * 3,
            out_specs=(anyspec,) * 3,
            scratch_shapes=[dma((3,))],
            compiler_params=pltpu.CompilerParams(vmem_limit_bytes=4 << 20),
        )(dq, dk, dv)
        return jnp.transpose(dq.reshape(heads, rows, head), (1, 0, 2)), dk, dv

    seq = P(("dp", "cpo", "cp"))
    return jax.shard_map(local, mesh=mesh, in_specs=(seq,) * 6 + (P("dp"),), out_specs=(seq, seq, seq), check_vma=False)
```

```python
import math

import jax
import jax.numpy as jnp
from jax import lax
from jax.experimental import pallas as pl
from jax.experimental.pallas import tpu as pltpu
from jax.sharding import PartitionSpec as P

ROWS = 512
HEADS = 3
DIM = 128
NBOUND = 14
QALL = HEADS * ROWS
XCH = 256
NX = ROWS // XCH
PCH = 128
LSIZE = (64, 64, 128, 96, 160)
LOFF = (0, 64, 128, 256, 352)
NL = len(LSIZE)
NRLY = 4
STEPS = tuple(zip(LOFF, LSIZE))
RLYROWS = sum(LSIZE[:NRLY])
LOG2E = math.log2(math.e)
MESH = pl.DeviceIdType.MESH
F32 = jnp.float32
BF16 = jnp.bfloat16
NT = (((1,), (1,)), ((), ()))
TN = (((0,), (0,)), ((), ()))


def device(rank):
    return (0, rank >> 2, rank & 3)


def kernel(cu_hbm, q_hbm, k_hbm, v_hbm, o_hbm, lse_hbm, do_hbm, dq_ref, dk_ref, dv_ref,
           cu_ref, qd, row, qfar, rfar, o_ref, lse_ref, kvown, kvx, kvl, kvb, dqt, own, mine, xout, lret, xret, rly,
           in_sem, out_sem, lend_r, kv_r, re_r, le_r, kx_r, xo_r):
    rank = lax.axis_index("cpo") * 4 + lax.axis_index("cp")
    core = rank & 1
    chip = rank >> 1
    sib = rank + 1 - 2 * core
    scale = DIM ** -0.5

    sems = (0, 0, 1, 1, 2, 3, 4)
    loads = [pltpu.make_async_copy(src, dst, in_sem.at[n]) for n, (src, dst) in zip(sems, [
        (k_hbm, kvown.at[0]), (v_hbm, kvown.at[1]), (do_hbm, qd.at[0, 1]), (q_hbm, qd.at[0, 0]), (o_hbm, o_ref),
        (lse_hbm, lse_ref), (cu_hbm, cu_ref)])]
    kv_loaded = pltpu.make_async_copy(kvown, kvown, in_sem.at[0])
    qd_loaded = pltpu.make_async_copy(qd.at[0], qd.at[0], in_sem.at[1])
    loads[0].start()
    loads[1].start()

    has_l = chip >= 1
    has_r = chip <= 2
    x_from = jnp.where(core == 1, rank - 1, rank - 3)
    x_to = jnp.where(core == 1, rank + 3, rank + 1)
    has_x = x_from >= 0
    x_ret = x_to <= 7

    barrier = pltpu.get_barrier_semaphore()

    def greet(other):
        pl.semaphore_signal(barrier, inc=1, device_id=device(other), device_id_type=MESH)

    far_right = (core == 1) & (chip <= 1)
    far_left = (core == 0) & (chip >= 2)
    left = sib - 2
    right = sib + 2
    pl.when(has_l)(lambda: greet(left))
    pl.when(has_r)(lambda: greet(right))
    pl.when(far_right)(lambda: greet(rank + 3))
    pl.when(far_left)(lambda: greet(rank - 3))
    pl.when(chip == 1)(lambda: greet(rank + 4))
    pl.when(chip == 3)(lambda: greet(rank - 4))
    pl.when(rank == 1)(lambda: greet(5))
    pl.when(rank == 5)(lambda: greet(1))
    greet(sib)
    for copy in loads[2:]:
        copy.start()
    one = jnp.int32(1)
    zero = jnp.int32(0)
    count = one
    for there in (has_l, has_r, far_right, far_left, chip == 1, chip == 3, rank == 1, rank == 5):
        count = count + jnp.where(there, one, zero)
    pl.semaphore_wait(barrier, count)

    def remote(src, dst, s_sem, r_sem, other):
        return pltpu.make_async_remote_copy(src_ref=src, dst_ref=dst, send_sem=s_sem, recv_sem=r_sem,
                                            device_id=device(other), device_id_type=MESH)

    def rows(off, size):
        return pl.ds(off, size)

    kv_s, kx_s, re_s, le_s, xo_s = in_sem.at[0], out_sem.at[0], out_sem.at[1], out_sem.at[2], out_sem.at[3]
    last = pl.ds(LOFF[-1], LSIZE[-1])
    whole = (NL, 0, ROWS)
    halves = ((0, 0, XCH), (NL - 1, XCH, XCH))

    def half_of(i):
        return min(i // 3, 1)

    def third(i):
        return min(max(i - 2, 0), 2)

    def lend(src, dst, s_n, r_n, other):
        return remote(src, dst, in_sem.at[s_n], lend_r.at[r_n], other)

    def kv_right(i, off, size):
        return remote(kvown.at[:, rows(off, size)], kvl.at[core, :, rows(off, size)], kv_s, kv_r.at[min(i, NL - 1)], right)

    def kv_in(i, off, size):
        return remote(kvown.at[:, rows(off, size)], kvl.at[1 - core, :, rows(off, size)], kv_s, kv_r.at[i], left)

    def bounce():
        return remote(kvown.at[:, last], kvb, kv_s, le_r.at[0], rank + 4)

    def bounce_on():
        return remote(kvb, kvl.at[core, :, last], kv_s, kv_r.at[NL - 1], left)

    def kv_relay(i, off, size):
        part = kvl.at[1 - core, :, rows(off, size)]
        return remote(part, part, re_s, re_r.at[half_of(i)], sib)

    def kv_relayed(i, off, size):
        part = kvl.at[core, :, rows(off, size)]
        return remote(part, part, re_s, re_r.at[half_of(i)], sib)

    def kv_x():
        return remote(kvown, kvx, kx_s, kx_r.at[0], x_to)

    def give_x():
        return remote(xout, xret, xo_s, xo_r.at[0], rank - 3)

    def give_left(i, off, size):
        return remote(mine.at[:, rows(off, size)], lret.at[:, rows(off, size)], le_s, le_r.at[third(i)], left)

    def give_relay(i, off, size):
        return remote(mine.at[:, rows(off, size)], rly.at[:, rows(off, size)], le_s, kv_r.at[i], 1)

    def pass_on(i, off, size):
        return remote(rly.at[:, rows(off, size)], lret.at[:, rows(off, size)], le_s, le_r.at[third(i)], 2)

    kv_loaded.wait()

    @pl.when(has_r)
    def _():
        pl.when(chip == 1)(lambda: bounce().start())
        for i in range(NL - 1):
            kv_right(i, LOFF[i], LSIZE[i]).start()
        pl.when(chip != 1)(lambda: kv_right(NL - 1, LOFF[-1], LSIZE[-1]).start())

    qd_loaded.wait()
    far_to = jnp.where(core == 0, rank - 3, rank + 3)
    sib_qd, sib_row = lend(qd.at[0], qd.at[1], 1, 0, sib), lend(row.at[0], row.at[1], 3, 1, sib)
    far_qd, far_row = lend(qd.at[0, :, :, 0:XCH], qfar, 4, 2, far_to), lend(rfar.at[0], rfar.at[1], 2, 3, far_to)
    loads[6].wait()
    pl.when(far_left)(lambda: far_qd.start())
    sib_qd.start()

    pos = rank * ROWS + lax.broadcasted_iota(jnp.int32, (1, ROWS), 1)
    start = jnp.zeros((1, ROWS), jnp.int32)
    for n in range(NBOUND):
        bound = cu_ref[n]
        start = jnp.where(bound <= pos, bound, start)
    loads[4].wait()
    loads[5].wait()
    for g in range(HEADS):
        lanes = slice(g * ROWS, (g + 1) * ROWS)
        prod = qd[0, 1, g].astype(F32) * o_ref[g].astype(F32)
        half = slice(g * XCH, (g + 1) * XCH)
        for n, line in enumerate([lse_ref[g:g + 1, :] * LOG2E, jnp.sum(prod.T, axis=0, keepdims=True), start.astype(F32)]):
            row[0, n:n + 1, lanes] = line
            rfar[0, n:n + 1, half] = line[:, 0:XCH]
    sib_row.start()
    pl.when(far_left)(lambda: far_row.start())

    def lines(ref, spans):
        return [jnp.concatenate([ref[n:n + 1, span] for span in spans], axis=1) for n in range(3)]

    def queries(who):
        return [qd[who, n].reshape(QALL, DIM) for n in range(2)] + [row[who, n:n + 1, :] for n in range(3)]

    def own_rows(lo, hi):
        q, do = (qd[0, n, :, lo:hi].reshape(HEADS * (hi - lo), DIM) for n in range(2))
        return [q, do] + lines(row.at[0], [slice(g * ROWS + lo, g * ROWS + hi) for g in range(HEADS)])

    def part(query, kv, off, size, first_key, low=None, dq_rows=None, want_kv=True):
        q, do, lse, dot, start = query
        k = kv[0, off:off + size, :]
        v = kv[1, off:off + size, :]
        width = q.shape[0]
        key = lax.broadcasted_iota(jnp.int32, (size, width), 0)
        keep = (first_key + off + key).astype(F32) >= start
        if low is not None:
            keep = keep & (key <= lax.rem(lax.broadcasted_iota(jnp.int32, (size, width), 1), ROWS - low))
        s = lax.dot_general(k, q, NT, preferred_element_type=F32)
        dp = lax.dot_general(v, do, NT, preferred_element_type=F32)
        p = jnp.exp2(s * (scale * LOG2E) - lse)
        p = jnp.where(keep, p, 0.0)
        ds = (p * (dp - dot)).astype(BF16)
        if dq_rows is not None:
            lo, hi = dq_rows
            dq = lax.dot_general(k, ds, TN, preferred_element_type=F32)
            if low == 0:
                dqt[...] = dq
            elif hi - lo == ROWS:
                dqt[...] += dq
            else:
                for g in range(HEADS):
                    dqt[:, g * ROWS + lo:g * ROWS + hi] += dq[:, g * (hi - lo):(g + 1) * (hi - lo)]
        if want_kv:
            dv = jnp.dot(p.astype(BF16), do, preferred_element_type=F32)
            dk = jnp.dot(ds, q, preferred_element_type=F32)
            return dk, dv

    everything = (0, ROWS)

    for off in range(0, ROWS, XCH):
        dk, dv = part(own_rows(off, ROWS), kvown, off, XCH, rank * ROWS, low=off, dq_rows=(off, ROWS))
        own[0, off:off + XCH] = dk
        own[1, off:off + XCH] = dv

    pl.when(x_ret)(lambda: kv_x().start())

    def fetch(n):
        kv_in(n, *STEPS[n]).wait_recv()
        kv_relay(n, *STEPS[n]).start()

    def lstep(n, fetched=False):
        off, size = STEPS[n]
        pieces = [(n, off, size)]
        if not fetched:
            fetch(n)
        mine_kv = kvl.at[1 - core]
        dk, dv = part(queries(0), mine_kv, off, size, left * ROWS, dq_rows=everything)
        if n == 0:
            @pl.when(rank != 4)
            def _():
                sib_qd.wait_recv()
                sib_row.wait_recv()
        dk2, dv2 = part(queries(1), mine_kv, off, size, left * ROWS)
        mine[0, off:off + size] = dk + dk2
        mine[1, off:off + size] = dv + dv2

        @pl.when(rank != 5)
        def _():
            for piece in pieces:
                give_left(*piece).start()

        if n < NRLY:
            pl.when(rank == 5)(lambda: give_relay(*pieces[0]).start())

    def sib_keys(off):
        dk, dv = part(queries(1), kvown, off, XCH, rank * ROWS)
        own[0, off:off + XCH] += dk
        own[1, off:off + XCH] += dv

    @pl.when(rank == 4)
    def _():
        sib_qd.wait_recv()
        sib_row.wait_recv()
        sib_keys(0)

    @pl.when(chip == 3)
    def _():
        bounce().wait_recv()
        bounce_on().start()

    @pl.when(has_l)
    def _():
        for n in range(NL - 2):
            lstep(n)
        pl.when(rank != 2)(lambda: lstep(NL - 2))

        @pl.when(rank == 2)
        def _():
            fetch(NL - 2)
            fetch(NL - 1)

    @pl.when(far_left)
    def _():
        kv_x().wait_recv()
        dk, dv = part(queries(0), kvx, XCH, XCH, x_from * ROWS, dq_rows=everything)
        xout[0] = dk
        xout[1] = dv
        give_x().start()

    pl.when(has_l & (rank != 2))(lambda: lstep(NL - 1))

    @pl.when(far_left)
    def _():
        part(own_rows(0, XCH), kvx, 0, XCH, x_from * ROWS, dq_rows=(0, XCH), want_kv=False)

    @pl.when(has_l)
    def _():
        for off in range(0, ROWS, XCH):
            kv_relayed(*halves[off // XCH]).wait_recv()
            part(queries(0), kvl.at[core], off, XCH, (rank - 2) * ROWS, dq_rows=everything, want_kv=False)
        pl.when(rank == 5)(lambda: give_left(NL - 1, *STEPS[-1]).start())

    @pl.when(chip == 0)
    def _():
        sib_qd.wait_recv()
        sib_row.wait_recv()

    @pl.when(core == 1)
    def _():
        kv_x().wait_recv()
        for i in range(NX):
            part(queries(0), kvx, i * XCH, XCH, x_from * ROWS, dq_rows=everything, want_kv=False)

    @pl.when(core == 0)
    def _():
        pl.when(rank != 4)(lambda: sib_keys(0))

        @pl.when(rank == 2)
        def _():
            lstep(NL - 2, fetched=True)
            lstep(NL - 1, fetched=True)

        sib_keys(XCH)

    @pl.when(far_right)
    def _():
        far_qd.wait_recv()
        far_row.wait_recv()
        far = [qfar[n].reshape(HEADS * XCH, DIM) for n in range(2)] + [rfar[1, n:n + 1, :] for n in range(3)]
        dk, dv = part(far, kvown, 0, XCH, rank * ROWS)
        own[0, 0:XCH] += dk
        own[1, 0:XCH] += dv

    @pl.when(rank == 1)
    def _():
        for i in range(NRLY):
            give_relay(i, LOFF[i], LSIZE[i]).wait_recv()
            pass_on(i, LOFF[i], LSIZE[i]).start()

    for g in range(HEADS):
        lanes = slice(g * ROWS, (g + 1) * ROWS)
        dq_ref[lanes] = (dqt[:, lanes].T * scale).astype(BF16)

    pl.when(has_r)(lambda: kv_right(*whole).wait_send())
    pl.when(chip == 3)(lambda: bounce_on().wait_send())
    pl.when(x_ret)(lambda: kv_x().wait_send())
    sib_qd.wait_send()
    sib_row.wait_send()

    @pl.when(far_left)
    def _():
        far_qd.wait_send()
        far_row.wait_send()
        give_x().wait_send()

    @pl.when(has_l)
    def _():
        kv_relay(*whole).wait_send()
        give_left(*whole).wait_send()

    pl.when(rank == 1)(lambda: pass_on(NL, 0, RLYROWS).wait_send())

    for i, off, size in ((0, 0, XCH), (3, LOFF[3], LSIZE[3]), (4, LOFF[4], LSIZE[4])):
        span = slice(off, off + size)

        if off == XCH:
            @pl.when(far_right)
            def _():
                give_x().wait_recv()
                own[:, XCH:] += xret[...]

        @pl.when(has_r)
        def _():
            give_left(i, off, size).wait_recv()
            dk_ref[span, :] = ((own[0, span] + lret[0, span]) * scale).astype(BF16)
            dv_ref[span, :] = (own[1, span] + lret[1, span]).astype(BF16)

        @pl.when(chip == 3)
        def _():
            dk_ref[span, :] = (own[0, span] * scale).astype(BF16)
            dv_ref[span, :] = own[1, span].astype(BF16)


def write_out(dq_ref, dk_ref, dv_ref, dq_hbm, dk_hbm, dv_hbm, sem):
    copies = [pltpu.make_async_copy(src, dst, sem.at[n]) for n, (src, dst) in enumerate([
        (dq_ref, dq_hbm), (dk_ref, dk_hbm), (dv_ref, dv_hbm)])]
    for copy in copies:
        copy.start()
    for copy in copies:
        copy.wait()


def solution(mesh):
    def local(queries, keys, values, attn_out, logsumexp, d_out, cu_seqlens):
        rows, heads, head = queries.shape
        flat = lambda a: jnp.transpose(a, (1, 0, 2))
        kv = pltpu.VMEM((2, rows, head), BF16)
        sums = pltpu.VMEM((2, rows, head), F32)
        row = pltpu.VMEM((2, 8, QALL), F32)
        qd = pltpu.VMEM((2, 2, heads, rows, head), BF16)
        xsum = pltpu.VMEM((2, XCH, head), F32)
        dma = pltpu.SemaphoreType.DMA
        anyspec = pl.BlockSpec(memory_space=pl.ANY)
        vspec = pl.BlockSpec(memory_space=pltpu.VMEM)
        dq, dk, dv = pl.pallas_call(
            kernel,
            out_shape=(pltpu.VMEM((QALL, head), BF16), pltpu.VMEM((rows, head), BF16), pltpu.VMEM((rows, head), BF16)),
            in_specs=[anyspec] * 7,
            out_specs=(vspec, vspec, vspec),
            scratch_shapes=[pltpu.SMEM((NBOUND,), jnp.int32), qd, row, pltpu.VMEM((2, heads, XCH, head), BF16),
                            pltpu.VMEM((2, 8, heads * XCH), F32), pltpu.VMEM((heads, rows, head), BF16),
                            pltpu.VMEM((heads, rows), F32), kv, kv, pltpu.VMEM((2, 2, rows, head), BF16),
                            pltpu.VMEM((2, LSIZE[-1], head), BF16),
                            pltpu.VMEM((head, QALL), F32), sums, sums, xsum, sums, xsum, sums,
                            dma((5,)), dma((4,)), dma((4,)), dma((NL,)), dma((2,)), dma((3,)), dma((1,)), dma((1,))],
            compiler_params=pltpu.CompilerParams(collective_id=0, has_side_effects=True,
                                                 vmem_limit_bytes=48 << 20),
        )(*[pltpu.with_memory_space_constraint(a, pltpu.HBM) for a in (
            cu_seqlens, flat(queries), keys, values, flat(attn_out), logsumexp.T, flat(d_out))])
        dq, dk, dv = pl.pallas_call(
            write_out,
            out_shape=(jax.ShapeDtypeStruct(dq.shape, BF16), jax.ShapeDtypeStruct(dk.shape, BF16),
                       jax.ShapeDtypeStruct(dv.shape, BF16)),
            in_specs=[vspec] * 3,
            out_specs=(anyspec,) * 3,
            scratch_shapes=[dma((3,))],
            compiler_params=pltpu.CompilerParams(vmem_limit_bytes=4 << 20),
        )(dq, dk, dv)
        return jnp.transpose(dq.reshape(heads, rows, head), (1, 0, 2)), dk, dv

    seq = P(("dp", "cpo", "cp"))
    return jax.shard_map(local, mesh=mesh, in_specs=(seq,) * 6 + (P("dp"),), out_specs=(seq, seq, seq), check_vma=False)
```

```python
import math

import jax
import jax.numpy as jnp
from jax import lax
from jax.experimental import pallas as pl
from jax.experimental.pallas import tpu as pltpu
from jax.sharding import PartitionSpec as P

ROWS = 512
HEADS = 3
DIM = 128
NBOUND = 14
QALL = HEADS * ROWS
XCH = 256
NX = ROWS // XCH
PCH = 128
LSIZE = (64, 64, 128, 96, 160)
LOFF = (0, 64, 128, 256, 352)
NL = len(LSIZE)
NRLY = 4
STEPS = tuple(zip(LOFF, LSIZE))
RLYROWS = sum(LSIZE[:NRLY])
LOG2E = math.log2(math.e)
MESH = pl.DeviceIdType.MESH
F32 = jnp.float32
BF16 = jnp.bfloat16
NT = (((1,), (1,)), ((), ()))
TN = (((0,), (0,)), ((), ()))


def device(rank):
    return (0, rank >> 2, rank & 3)


def kernel(cu_hbm, q_hbm, k_hbm, v_hbm, o_hbm, lse_hbm, do_hbm, dq_ref, dk_ref, dv_ref,
           cu_ref, qd, row, qfar, rfar, o_ref, lse_ref, kvown, kvx, kvl, kvb, dqt, own, mine, xout, lret, xret, rly,
           in_sem, out_sem, lend_r, kv_r, re_r, le_r, kx_r, xo_r):
    rank = lax.axis_index("cpo") * 4 + lax.axis_index("cp")
    core = rank & 1
    chip = rank >> 1
    sib = rank + 1 - 2 * core
    scale = DIM ** -0.5

    sems = (0, 0, 1, 1, 2, 3, 4)
    loads = [pltpu.make_async_copy(src, dst, in_sem.at[n]) for n, (src, dst) in zip(sems, [
        (k_hbm, kvown.at[0]), (v_hbm, kvown.at[1]), (do_hbm, qd.at[0, 1]), (q_hbm, qd.at[0, 0]), (o_hbm, o_ref),
        (lse_hbm, lse_ref), (cu_hbm, cu_ref)])]
    kv_loaded = pltpu.make_async_copy(kvown, kvown, in_sem.at[0])
    qd_loaded = pltpu.make_async_copy(qd.at[0], qd.at[0], in_sem.at[1])
    loads[0].start()
    loads[1].start()

    has_l = chip >= 1
    has_r = chip <= 2
    x_from = jnp.where(core == 1, rank - 1, rank - 3)
    x_to = jnp.where(core == 1, rank + 3, rank + 1)
    has_x = x_from >= 0
    x_ret = x_to <= 7

    barrier = pltpu.get_barrier_semaphore()

    def greet(other):
        pl.semaphore_signal(barrier, inc=1, device_id=device(other), device_id_type=MESH)

    far_right = (core == 1) & (chip <= 1)
    far_left = (core == 0) & (chip >= 2)
    left = sib - 2
    right = sib + 2
    pl.when(has_l)(lambda: greet(left))
    pl.when(has_r)(lambda: greet(right))
    pl.when(far_right)(lambda: greet(rank + 3))
    pl.when(far_left)(lambda: greet(rank - 3))
    pl.when(chip == 1)(lambda: greet(rank + 4))
    pl.when(chip == 3)(lambda: greet(rank - 4))
    pl.when(rank == 1)(lambda: greet(5))
    pl.when(rank == 5)(lambda: greet(1))
    greet(sib)
    for copy in loads[2:]:
        copy.start()
    one = jnp.int32(1)
    zero = jnp.int32(0)
    count = one
    for there in (has_l, has_r, far_right, far_left, chip == 1, chip == 3, rank == 1, rank == 5):
        count = count + jnp.where(there, one, zero)
    pl.semaphore_wait(barrier, count)

    def remote(src, dst, s_sem, r_sem, other):
        return pltpu.make_async_remote_copy(src_ref=src, dst_ref=dst, send_sem=s_sem, recv_sem=r_sem,
                                            device_id=device(other), device_id_type=MESH)

    def rows(off, size):
        return pl.ds(off, size)

    kv_s, kx_s, re_s, le_s, xo_s = in_sem.at[0], in_sem.at[3], in_sem.at[1], out_sem.at[0], in_sem.at[4]
    last = pl.ds(LOFF[-1], LSIZE[-1])
    whole = (NL, 0, ROWS)
    halves = ((0, 0, XCH), (NL - 1, XCH, XCH))

    def half_of(i):
        return min(i // 3, 1)

    def third(i):
        return min(max(i - 2, 0), 2)

    def lend(src, dst, s_n, r_n, other):
        return remote(src, dst, in_sem.at[s_n], lend_r.at[r_n], other)

    def kv_right(i, off, size):
        return remote(kvown.at[:, rows(off, size)], kvl.at[core, :, rows(off, size)], kv_s, kv_r.at[min(i, NL - 1)], right)

    def kv_in(i, off, size):
        return remote(kvown.at[:, rows(off, size)], kvl.at[1 - core, :, rows(off, size)], kv_s, kv_r.at[i], left)

    def bounce():
        return remote(kvown.at[:, last], kvb, kv_s, le_r.at[0], rank + 4)

    def bounce_on():
        return remote(kvb, kvl.at[core, :, last], kv_s, kv_r.at[NL - 1], left)

    def kv_relay(i, off, size):
        part = kvl.at[1 - core, :, rows(off, size)]
        return remote(part, part, re_s, re_r.at[half_of(i)], sib)

    def kv_relayed(i, off, size):
        part = kvl.at[core, :, rows(off, size)]
        return remote(part, part, re_s, re_r.at[half_of(i)], sib)

    def kv_x():
        return remote(kvown, kvx, kx_s, kx_r.at[0], x_to)

    def give_x():
        return remote(xout, xret, xo_s, xo_r.at[0], rank - 3)

    def give_left(i, off, size):
        return remote(mine.at[:, rows(off, size)], lret.at[:, rows(off, size)], le_s, le_r.at[third(i)], left)

    def give_relay(i, off, size):
        return remote(mine.at[:, rows(off, size)], rly.at[:, rows(off, size)], le_s, kv_r.at[i], 1)

    def pass_on(i, off, size):
        return remote(rly.at[:, rows(off, size)], lret.at[:, rows(off, size)], le_s, le_r.at[third(i)], 2)

    kv_loaded.wait()

    @pl.when(has_r)
    def _():
        pl.when(chip == 1)(lambda: bounce().start())
        for i in range(NL - 1):
            kv_right(i, LOFF[i], LSIZE[i]).start()
        pl.when(chip != 1)(lambda: kv_right(NL - 1, LOFF[-1], LSIZE[-1]).start())

    qd_loaded.wait()
    far_to = jnp.where(core == 0, rank - 3, rank + 3)
    sib_qd, sib_row = lend(qd.at[0], qd.at[1], 1, 0, sib), lend(row.at[0], row.at[1], 3, 1, sib)
    far_qd, far_row = lend(qd.at[0, :, :, 0:XCH], qfar, 4, 2, far_to), lend(rfar.at[0], rfar.at[1], 2, 3, far_to)
    loads[6].wait()
    pl.when(far_left)(lambda: far_qd.start())
    sib_qd.start()

    pos = rank * ROWS + lax.broadcasted_iota(jnp.int32, (1, ROWS), 1)
    start = jnp.zeros((1, ROWS), jnp.int32)
    for n in range(NBOUND):
        bound = cu_ref[n]
        start = jnp.where(bound <= pos, bound, start)
    loads[4].wait()
    loads[5].wait()
    for g in range(HEADS):
        lanes = slice(g * ROWS, (g + 1) * ROWS)
        prod = qd[0, 1, g].astype(F32) * o_ref[g].astype(F32)
        half = slice(g * XCH, (g + 1) * XCH)
        for n, line in enumerate([lse_ref[g:g + 1, :] * LOG2E, jnp.sum(prod.T, axis=0, keepdims=True), start.astype(F32)]):
            row[0, n:n + 1, lanes] = line
            rfar[0, n:n + 1, half] = line[:, 0:XCH]
    sib_row.start()
    pl.when(far_left)(lambda: far_row.start())

    def lines(ref, spans):
        return [jnp.concatenate([ref[n:n + 1, span] for span in spans], axis=1) for n in range(3)]

    def queries(who):
        return [qd[who, n].reshape(QALL, DIM) for n in range(2)] + [row[who, n:n + 1, :] for n in range(3)]

    def own_rows(lo, hi):
        q, do = (qd[0, n, :, lo:hi].reshape(HEADS * (hi - lo), DIM) for n in range(2))
        return [q, do] + lines(row.at[0], [slice(g * ROWS + lo, g * ROWS + hi) for g in range(HEADS)])

    def part(query, kv, off, size, first_key, low=None, dq_rows=None, want_kv=True):
        q, do, lse, dot, start = query
        k = kv[0, off:off + size, :]
        v = kv[1, off:off + size, :]
        width = q.shape[0]
        key = lax.broadcasted_iota(jnp.int32, (size, width), 0)
        keep = (first_key + off + key).astype(F32) >= start
        if low is not None:
            keep = keep & (key <= lax.rem(lax.broadcasted_iota(jnp.int32, (size, width), 1), ROWS - low))
        s = lax.dot_general(k, q, NT, preferred_element_type=F32)
        dp = lax.dot_general(v, do, NT, preferred_element_type=F32)
        p = jnp.exp2(s * (scale * LOG2E) - lse)
        p = jnp.where(keep, p, 0.0)
        ds = (p * (dp - dot)).astype(BF16)
        if dq_rows is not None:
            lo, hi = dq_rows
            dq = lax.dot_general(k, ds, TN, preferred_element_type=F32)
            if low == 0:
                dqt[...] = dq
            elif hi - lo == ROWS:
                dqt[...] += dq
            else:
                for g in range(HEADS):
                    dqt[:, g * ROWS + lo:g * ROWS + hi] += dq[:, g * (hi - lo):(g + 1) * (hi - lo)]
        if want_kv:
            dv = jnp.dot(p.astype(BF16), do, preferred_element_type=F32)
            dk = jnp.dot(ds, q, preferred_element_type=F32)
            return dk, dv

    everything = (0, ROWS)

    for off in range(0, ROWS, XCH):
        dk, dv = part(own_rows(off, ROWS), kvown, off, XCH, rank * ROWS, low=off, dq_rows=(off, ROWS))
        own[0, off:off + XCH] = dk
        own[1, off:off + XCH] = dv

    sib_row.wait_send()
    sib_qd.wait_send()
    pl.when(x_ret)(lambda: kv_x().start())

    def fetch(n):
        kv_in(n, *STEPS[n]).wait_recv()
        kv_relay(n, *STEPS[n]).start()

    def lstep(n, fetched=False):
        off, size = STEPS[n]
        pieces = [(n, off, size)]
        if not fetched:
            fetch(n)
        mine_kv = kvl.at[1 - core]
        dk, dv = part(queries(0), mine_kv, off, size, left * ROWS, dq_rows=everything)
        if n == 0:
            @pl.when(rank != 4)
            def _():
                sib_qd.wait_recv()
                sib_row.wait_recv()
        dk2, dv2 = part(queries(1), mine_kv, off, size, left * ROWS)
        mine[0, off:off + size] = dk + dk2
        mine[1, off:off + size] = dv + dv2

        @pl.when(rank != 5)
        def _():
            for piece in pieces:
                give_left(*piece).start()

        if n < NRLY:
            pl.when(rank == 5)(lambda: give_relay(*pieces[0]).start())

    def sib_keys(off):
        dk, dv = part(queries(1), kvown, off, XCH, rank * ROWS)
        own[0, off:off + XCH] += dk
        own[1, off:off + XCH] += dv

    @pl.when(rank == 4)
    def _():
        sib_qd.wait_recv()
        sib_row.wait_recv()
        sib_keys(0)

    @pl.when(chip == 3)
    def _():
        bounce().wait_recv()
        bounce_on().start()

    @pl.when(has_l)
    def _():
        for n in range(NL - 2):
            lstep(n)
        pl.when(rank != 2)(lambda: lstep(NL - 2))

        @pl.when(rank == 2)
        def _():
            fetch(NL - 2)
            fetch(NL - 1)

    @pl.when(far_left)
    def _():
        kv_x().wait_recv()
        dk, dv = part(queries(0), kvx, XCH, XCH, x_from * ROWS, dq_rows=everything)
        xout[0] = dk
        xout[1] = dv
        far_qd.wait_send()
        give_x().start()

    pl.when(has_l & (rank != 2))(lambda: lstep(NL - 1))

    @pl.when(far_left)
    def _():
        part(own_rows(0, XCH), kvx, 0, XCH, x_from * ROWS, dq_rows=(0, XCH), want_kv=False)

    @pl.when(has_l)
    def _():
        for off in range(0, ROWS, XCH):
            kv_relayed(*halves[off // XCH]).wait_recv()
            part(queries(0), kvl.at[core], off, XCH, (rank - 2) * ROWS, dq_rows=everything, want_kv=False)
        pl.when(rank == 5)(lambda: give_left(NL - 1, *STEPS[-1]).start())

    @pl.when(chip == 0)
    def _():
        sib_qd.wait_recv()
        sib_row.wait_recv()

    @pl.when(core == 1)
    def _():
        kv_x().wait_recv()
        for i in range(NX):
            part(queries(0), kvx, i * XCH, XCH, x_from * ROWS, dq_rows=everything, want_kv=False)

    @pl.when(core == 0)
    def _():
        pl.when(rank != 4)(lambda: sib_keys(0))

        @pl.when(rank == 2)
        def _():
            lstep(NL - 2, fetched=True)
            lstep(NL - 1, fetched=True)

        sib_keys(XCH)

    @pl.when(far_right)
    def _():
        far_qd.wait_recv()
        far_row.wait_recv()
        far = [qfar[n].reshape(HEADS * XCH, DIM) for n in range(2)] + [rfar[1, n:n + 1, :] for n in range(3)]
        dk, dv = part(far, kvown, 0, XCH, rank * ROWS)
        own[0, 0:XCH] += dk
        own[1, 0:XCH] += dv

    @pl.when(rank == 1)
    def _():
        for i in range(NRLY):
            give_relay(i, LOFF[i], LSIZE[i]).wait_recv()
            pass_on(i, LOFF[i], LSIZE[i]).start()

    for g in range(HEADS):
        lanes = slice(g * ROWS, (g + 1) * ROWS)
        dq_ref[lanes] = (dqt[:, lanes].T * scale).astype(BF16)

    pl.when(has_r)(lambda: kv_right(*whole).wait_send())
    pl.when(chip == 3)(lambda: bounce_on().wait_send())
    pl.when(x_ret)(lambda: kv_x().wait_send())

    @pl.when(far_left)
    def _():
        far_row.wait_send()
        give_x().wait_send()

    @pl.when(has_l)
    def _():
        kv_relay(*whole).wait_send()
        give_left(*whole).wait_send()

    pl.when(rank == 1)(lambda: pass_on(NL, 0, RLYROWS).wait_send())

    for i, off, size in ((0, 0, XCH), (3, LOFF[3], LSIZE[3]), (4, LOFF[4], LSIZE[4])):
        span = slice(off, off + size)

        if off == XCH:
            @pl.when(far_right)
            def _():
                give_x().wait_recv()
                own[:, XCH:] += xret[...]

        @pl.when(has_r)
        def _():
            give_left(i, off, size).wait_recv()
            dk_ref[span, :] = ((own[0, span] + lret[0, span]) * scale).astype(BF16)
            dv_ref[span, :] = (own[1, span] + lret[1, span]).astype(BF16)

        @pl.when(chip == 3)
        def _():
            dk_ref[span, :] = (own[0, span] * scale).astype(BF16)
            dv_ref[span, :] = own[1, span].astype(BF16)


def write_out(dq_ref, dk_ref, dv_ref, dq_hbm, dk_hbm, dv_hbm, sem):
    copies = [pltpu.make_async_copy(src, dst, sem.at[n]) for n, (src, dst) in enumerate([
        (dq_ref, dq_hbm), (dk_ref, dk_hbm), (dv_ref, dv_hbm)])]
    for copy in copies:
        copy.start()
    for copy in copies:
        copy.wait()


def solution(mesh):
    def local(queries, keys, values, attn_out, logsumexp, d_out, cu_seqlens):
        rows, heads, head = queries.shape
        flat = lambda a: jnp.transpose(a, (1, 0, 2))
        kv = pltpu.VMEM((2, rows, head), BF16)
        sums = pltpu.VMEM((2, rows, head), F32)
        row = pltpu.VMEM((2, 8, QALL), F32)
        qd = pltpu.VMEM((2, 2, heads, rows, head), BF16)
        xsum = pltpu.VMEM((2, XCH, head), F32)
        dma = pltpu.SemaphoreType.DMA
        anyspec = pl.BlockSpec(memory_space=pl.ANY)
        vspec = pl.BlockSpec(memory_space=pltpu.VMEM)
        dq, dk, dv = pl.pallas_call(
            kernel,
            out_shape=(pltpu.VMEM((QALL, head), BF16), pltpu.VMEM((rows, head), BF16), pltpu.VMEM((rows, head), BF16)),
            in_specs=[anyspec] * 7,
            out_specs=(vspec, vspec, vspec),
            scratch_shapes=[pltpu.SMEM((NBOUND,), jnp.int32), qd, row, pltpu.VMEM((2, heads, XCH, head), BF16),
                            pltpu.VMEM((2, 8, heads * XCH), F32), pltpu.VMEM((heads, rows, head), BF16),
                            pltpu.VMEM((heads, rows), F32), kv, kv, pltpu.VMEM((2, 2, rows, head), BF16),
                            pltpu.VMEM((2, LSIZE[-1], head), BF16),
                            pltpu.VMEM((head, QALL), F32), sums, sums, xsum, sums, xsum, sums,
                            dma((5,)), dma((1,)), dma((4,)), dma((NL,)), dma((2,)), dma((3,)), dma((1,)), dma((1,))],
            compiler_params=pltpu.CompilerParams(collective_id=0, has_side_effects=True,
                                                 vmem_limit_bytes=48 << 20),
        )(*[pltpu.with_memory_space_constraint(a, pltpu.HBM) for a in (
            cu_seqlens, flat(queries), keys, values, flat(attn_out), logsumexp.T, flat(d_out))])
        dq, dk, dv = pl.pallas_call(
            write_out,
            out_shape=(jax.ShapeDtypeStruct(dq.shape, BF16), jax.ShapeDtypeStruct(dk.shape, BF16),
                       jax.ShapeDtypeStruct(dv.shape, BF16)),
            in_specs=[vspec] * 3,
            out_specs=(anyspec,) * 3,
            scratch_shapes=[dma((3,))],
            compiler_params=pltpu.CompilerParams(vmem_limit_bytes=4 << 20),
        )(dq, dk, dv)
        return jnp.transpose(dq.reshape(heads, rows, head), (1, 0, 2)), dk, dv

    seq = P(("dp", "cpo", "cp"))
    return jax.shard_map(local, mesh=mesh, in_specs=(seq,) * 6 + (P("dp"),), out_specs=(seq, seq, seq), check_vma=False)
```
